32 devices in a mesh: groups: 2 (over y), ctx: 8 (over z, x), head: 2 (over core).
Axes of the slice: x: 2, y: 2, z: 4, core: 2. Of those that a mesh axis runs over, the one named last changes fastest.
Arguments:
- query_latent: bfloat16 [16, 64, 576], P(('groups', 'ctx'), 'head'), parts along dimension 0, may hold values from -9 to 9
- latent_codes: bfloat16 [4096, 576], P(('groups', 'ctx')), parts along dimension 0, may hold values from -6 to 6
- latent_scales: float32 [4096, 9], P(('groups', 'ctx')), parts along dimension 0, may hold values from 0.5 to 2
- valid_lengths: int32 [16], P(('groups', 'ctx')), parts along dimension 0, may hold values from 1 to 256
- query_position: int32 [16], P('groups'), parts along dimension 0, may hold values from 0 to 2047
- value_up: bfloat16 [64, 512, 128], P('head'), may hold values from -1 to 1
- out_codes: bfloat16 [8192, 7168], P('head', 'ctx'), may hold values from -0.0625 to 0.0625
- out_scales: float32 [7168], P('ctx'), may hold values from 0.5 to 2
Outputs:
- attention: bfloat16 [16, 8192], P(('groups', 'ctx'), 'head'), parts along dimension 0
- projected: bfloat16 [16, 7168], P(('groups', 'head'), 'ctx'), parts along dimension 0
The draws below stay inside these ranges and needn't reach their ends.
There are 2 independent parts, one for each index of `groups`. The reference program is written for one: setup_inputs(seed, part) draws one part's arguments, and reference() takes and returns one part's arrays. A program takes and returns all parts, laid end to end along the dimension named above; an argument that names none is the same for every part. Nothing has to cross between parts.
All inputs are finite; a program needn't handle non-finite values.
Results may differ from the reference program's by a relative error of at most 0.011.
Values may be sent and summed in bfloat16 or wider, within the bound.
A program may use at most 128 MiB of HBM per device.

```python
import math
import jax
import jax.numpy as jnp
from jax import lax

D = 7168
LAT_NOPE = 512
ROPE = 64
VHEAD = 128
QK_NOPE = 128
HEADS = 64
SBLK = 64
CTX_DEV = 256
LAT = 576
NBLK = 9
CONTEXT = 2048
QTOK = 8
RANKS = 8
N_CTX = 8


def draw_latent_codes(key, part):
    codes = jnp.clip(jax.random.normal(jax.random.fold_in(key, 201), (CONTEXT, LAT), jnp.float32), -6.0, 6.0)
    return codes.astype(jnp.bfloat16)


def draw_query_latent(key, part):
    values = jnp.clip(1.5 * jax.random.normal(jax.random.fold_in(key, 301), (QTOK, HEADS, LAT), jnp.float32), -9.0, 9.0)
    return values.astype(jnp.bfloat16)


def place_ends(entries, own_key, low, top_value):
    longest = entries.shape.index(max(entries.shape))
    spots = []
    for shift in (0, 1):
        where = [jax.random.randint(jax.random.fold_in(own_key, axis), (), 0, length) for axis, length in enumerate(entries.shape)]
        where[longest] = (where[longest] + shift) % entries.shape[longest]
        spots.append(tuple(where))
    return entries.at[spots[0]].set(low).at[spots[1]].set(top_value)


def level_of(key, shape, pieces, smallest, top_value):
    loudness, own = 1.0, jax.random.fold_in(key, 6)
    for dim, shards_of in pieces:
        draws = jnp.exp(jax.random.uniform(jax.random.fold_in(own, dim), (shards_of,), jnp.float32, smallest / len(pieces), top_value / len(pieces)))
        loudness = loudness * jnp.repeat(draws, shape[dim] // shards_of).reshape([-1 if axis == dim else 1 for axis in range(len(shape))])
    return loudness


def gaussian(key, dims, width, reach, split=(), kind=jnp.bfloat16):
    level = level_of(key, dims, split, -0.22, 0.18) if split else 1.0
    drawn = jax.random.normal(key, dims, jnp.float32) * width * level
    return jnp.minimum(jnp.maximum(drawn, -reach), reach).astype(kind)


def setup_inputs(seed: int = 0, part: int = 0) -> dict:
    streams_of = jax.random.split(jax.random.key(seed), 9)
    part_keys = jax.random.split(jax.random.fold_in(streams_of[8], part), 9)
    query_latent = draw_query_latent(jax.random.fold_in(jax.random.fold_in(streams_of[8], part), 71), part)
    latent_codes = draw_latent_codes(jax.random.fold_in(jax.random.fold_in(streams_of[8], part), 71), part)
    latent_scales = jnp.clip(jnp.exp(math.log(2.0) - 1.3862944 * jax.random.uniform(part_keys[2], (CONTEXT, NBLK), jnp.float32) ** level_of(part_keys[2], (CONTEXT, NBLK), ((0, 8),), -0.2, 0.2)), 0.5, 2.0)
    valid_lengths = place_ends(jax.random.randint(part_keys[3], (RANKS,), 1, CTX_DEV + 1), jax.random.fold_in(part_keys[3], 1), 1, CTX_DEV).astype(jnp.int32)
    query_position = place_ends(jax.random.randint(part_keys[4], (QTOK,), 0, CONTEXT), jax.random.fold_in(part_keys[4], 1), 0, CONTEXT - 1).astype(jnp.int32)
    value_up = gaussian(streams_of[5], (HEADS, LAT_NOPE, VHEAD), (LAT_NOPE // 16) ** -0.5, 1.0, ((0, 2),))
    out_codes = gaussian(streams_of[6], (HEADS * VHEAD, D), (HEADS * VHEAD) ** -0.5, 0.0625, ((0, 2), (1, 8)))
    out_scales = jnp.clip(jnp.exp(math.log(2.0) - 1.3862944 * jax.random.uniform(streams_of[7], (D,), jnp.float32) ** level_of(streams_of[7], (D,), ((0, 8),), -0.2, 0.2)), 0.5, 2.0)
    return dict(query_latent=query_latent, latent_codes=latent_codes, latent_scales=latent_scales, valid_lengths=valid_lengths, query_position=query_position, value_up=value_up, out_codes=out_codes, out_scales=out_scales)


def reference(query_latent, latent_codes, latent_scales, valid_lengths, query_position, value_up, out_codes, out_scales):
    latent = (latent_codes.astype(jnp.float32).reshape(CONTEXT, NBLK, SBLK) * latent_scales[:, :, None]).reshape(CONTEXT, LAT).astype(jnp.bfloat16)
    key_pos = jnp.arange(CONTEXT, dtype=jnp.int32)
    owner = key_pos // CTX_DEV
    usable = (key_pos % CTX_DEV) < valid_lengths[owner]
    allowed = usable[None, :] & (key_pos[None, :] <= query_position[:, None])
    softmax_scale = (QK_NOPE + ROPE) ** -0.5
    nope_shards = latent[:, :LAT_NOPE].astype(jnp.float32).reshape(N_CTX, CTX_DEV, LAT_NOPE)

    def one_head(inputs):
        query_head, up_head = inputs
        logits = jnp.dot(query_head, latent.T, preferred_element_type=jnp.float32) * softmax_scale
        logits = jnp.where(allowed, logits, -jnp.inf)
        maxima = jnp.max(logits, axis=1, keepdims=True)
        weights = jnp.exp(logits - maxima)
        totals = jnp.sum(weights, axis=1)
        rounded = lax.optimization_barrier(weights.astype(jnp.bfloat16))
        rounded = rounded.astype(jnp.float32).reshape(QTOK, N_CTX, CTX_DEV)
        partial_mix = lax.optimization_barrier(jnp.einsum("qrk,rkd->rqd", rounded, nope_shards).astype(jnp.bfloat16))
        numerators = jnp.einsum("rqd,dv->qv", partial_mix.astype(jnp.float32), up_head.astype(jnp.float32))
        return numerators / totals[:, None]

    head_outputs = lax.map(one_head, (jnp.transpose(query_latent, (1, 0, 2)), value_up))
    attention = jnp.transpose(head_outputs, (1, 0, 2)).reshape(QTOK, HEADS * VHEAD).astype(jnp.bfloat16)
    projected = (jnp.dot(attention, out_codes, preferred_element_type=jnp.float32) * out_scales[None, :]).astype(jnp.bfloat16)
    return attention, projected
```

```python
import functools
import math

import jax
import jax.numpy as jnp
from jax import lax
from jax.experimental import pallas as pl
from jax.experimental.pallas import tpu as pltpu
from jax.sharding import PartitionSpec as P

LAT_NOPE = 512
ROPE = 64
QK_NOPE = 128
LANES = 128
MASKED = -1e30
MESH = pl.DeviceIdType.MESH


def shards(
    query_latent,
    latent_codes,
    latent_scales,
    valid_lengths,
    query_position,
    value_up,
    out_codes,
    out_scales,
):
    key_count, width = latent_codes.shape
    block_count = latent_scales.shape[1]
    latent = (
        (
            latent_codes.astype(jnp.float32).reshape(key_count, block_count, width // block_count)
            * latent_scales[:, :, None]
        )
        .reshape(key_count, width)
        .astype(jnp.bfloat16)
    )
    shard_index = lax.axis_index("ctx")
    local_slots = jnp.arange(key_count, dtype=jnp.int32)
    key_pos = shard_index * key_count + local_slots
    usable = local_slots < valid_lengths[0]
    softmax_scale = (QK_NOPE + ROPE) ** (-0.5)
    logits = (
        jnp.einsum(
            "qhc,kc->qhk",
            lax.all_gather(query_latent, "ctx", axis=0, tiled=True),
            latent,
            preferred_element_type=jnp.float32,
        )
        * softmax_scale
    )
    allowed = usable[None, :] & (key_pos[None, :] <= query_position[:, None])
    scores = jnp.where(allowed[:, None, :], logits, -jnp.inf)
    maxima = lax.pmax(jnp.max(scores, axis=2), "ctx")
    weights = jnp.exp(scores - maxima[:, :, None])
    totals = jnp.sum(weights, axis=2)
    latent_mix = jnp.einsum(
        "qhk,kd->qhd",
        weights.astype(jnp.bfloat16),
        latent[:, :LAT_NOPE],
        preferred_element_type=jnp.float32,
    ).astype(jnp.bfloat16)
    values = jnp.einsum("qhd,hdv->qhv", latent_mix, value_up, preferred_element_type=jnp.float32)
    queries, head_count, value_width = values.shape
    numerators = values.reshape(queries, head_count * value_width)
    own_rows = query_latent.shape[0]
    numer_sum, denom_sum = lax.psum((numerators, totals), "ctx")
    attn_all = (
        (numer_sum.reshape(queries, head_count, value_width) / denom_sum[:, :, None])
        .reshape(queries, head_count * value_width)
        .astype(jnp.bfloat16)
    )
    attn_home = lax.dynamic_slice_in_dim(attn_all, shard_index * own_rows, own_rows, 0)
    summed = lax.psum_scatter(
        jnp.dot(attn_all, out_codes, preferred_element_type=jnp.float32),
        "head",
        scatter_dimension=0,
        tiled=True,
    )
    projected = (summed * out_scales[None, :]).astype(jnp.bfloat16)
    return (attn_home, projected)


def flip(index, mask):
    bit, result = 1, index
    while bit <= mask:
        if mask & bit:
            result = result + bit - 2 * bit * lax.rem(index // bit, 2)
        bit *= 2
    return result


def fused(
    n,
    heads,
    valid_hbm,
    qpos_hbm,
    query_hbm,
    codes_hbm,
    scales_hbm,
    up_hbm,
    out_hbm,
    attn_ref,
    proj_ref,
    valid,
    qpos,
    near_valid,
    q_all,
    codes,
    near_codes,
    scales,
    near_scales,
    up,
    outw,
    latent,
    near_latent,
    mix,
    stat_m,
    stat_l,
    num_send,
    num_recv,
    st_send,
    st_recv,
    att_all,
    part,
    part_recv,
    ready,
    in_sem,
    up_sem,
    out_sem,
    q_ssem,
    q_rsem,
    near_ssem,
    near_rsem,
    half_ssem,
    half_rsem,
    num_ssem,
    num_rsem,
    st_ssem,
    st_rsem,
    att_ssem,
    att_rsem,
    part_ssem,
    part_rsem,
):
    me = lax.axis_index("ctx")
    hd = lax.axis_index("head")
    other = 1 - hd
    row, column = me // 2, lax.rem(me, 2)
    rows = n // 2
    head_count, width = q_all.shape[1:]
    pieces, piece, keys = codes.shape
    each = pieces // heads
    nope = mix.shape[0] * LANES
    vhead = up.shape[2]
    twin = head_count // 2
    per = twin // rows
    lines = 2 * rows

    barrier = pltpu.get_barrier_semaphore()
    for k in range(n - 1, 0, -1):
        later = flip(me, k)

        @pl.when(later > me)
        def _():
            pl.semaphore_signal(barrier, inc=1, device_id={"ctx": later}, device_id_type=MESH)

    pl.semaphore_signal(barrier, inc=1, device_id={"head": other}, device_id_type=MESH)

    loads = [
        pltpu.make_async_copy(codes_hbm, codes, in_sem.at[0]),
        pltpu.make_async_copy(scales_hbm, scales, in_sem.at[1]),
        pltpu.make_async_copy(query_hbm.at[0], q_all.at[row], in_sem.at[2]),
        pltpu.make_async_copy(valid_hbm, valid, in_sem.at[3]),
        pltpu.make_async_copy(qpos_hbm, qpos, in_sem.at[4]),
    ]
    for copy in loads:
        copy.start()

    pl.semaphore_wait(barrier, me + heads - 1)

    for k in range(1, n):
        earlier = flip(me, k)

        @pl.when(earlier < me)
        def _():
            pl.semaphore_signal(ready.at[k], inc=1, device_id={"ctx": earlier}, device_id_type=MESH)

    def admit(k):
        @pl.when(flip(me, k) > me)
        def _():
            pl.semaphore_wait(ready.at[k], 1)

    def remote(src, dst, ssem, rsem, **device):
        copy = pltpu.make_async_remote_copy(
            src_ref=src,
            dst_ref=dst,
            send_sem=ssem,
            recv_sem=rsem,
            device_id=device,
            device_id_type=MESH,
        )
        copy.start()
        return copy

    admit(1)
    partner = flip(me, 1)
    near = [
        remote(
            codes_hbm.at[hd * each + i],
            near_codes.at[hd * each + i],
            near_ssem.at[i],
            near_rsem.at[i],
            ctx=partner,
        )
        for i in range(each)
    ]
    near.append(remote(scales_hbm, near_scales, near_ssem.at[each], near_rsem.at[each], ctx=partner))
    near.append(remote(valid_hbm, near_valid, near_ssem.at[each + 1], near_rsem.at[each + 1], ctx=partner))

    up_in = []
    for g in range(2):
        part_of = pl.ds(g * twin, twin)
        up_in.append(pltpu.make_async_copy(up_hbm.at[part_of], up.at[part_of], up_sem.at[g]))
        up_in[-1].start()

    queries = []
    for k in range(1, rows):
        admit(2 * k)
        queries.append(
            remote(query_hbm.at[0], q_all.at[row], q_ssem.at[k], q_rsem.at[k], ctx=flip(me, 2 * k))
        )

    out_in = []
    half = outw.shape[0] // 2
    for g in range(2):
        part_of = pl.ds(g * half, half)
        out_in.append(pltpu.make_async_copy(out_hbm.at[part_of], outw.at[part_of], out_sem.at[g]))
        out_in[-1].start()

    block = width // scales.shape[0]

    def scale_latent(source, factors, target):
        unit = math.gcd(piece, block)
        for p in range(pieces):
            for r in range(0, piece, unit):
                at = p * piece + r
                b = at // block
                target[at : at + unit, :] = (
                    source[p, r : r + unit, :].astype(jnp.float32) * factors[b : b + 1, :]
                ).astype(jnp.bfloat16)

    for copy in loads:
        copy.wait()
    scale_latent(codes, scales, latent)

    relayed = []
    for i in range(each):
        near[i].wait_recv()
        relayed.append(
            remote(
                near_codes.at[hd * each + i],
                near_codes.at[hd * each + i],
                half_ssem.at[i],
                half_rsem.at[i],
                head=other,
            )
        )
    for copy in near[each:]:
        copy.wait_recv()
    for copy in queries:
        copy.wait_recv()
    for copy in relayed:
        copy.wait_recv()
    scale_latent(near_codes, near_scales, near_latent)

    softmax_scale = (QK_NOPE + ROPE) ** (-0.5)
    query = q_all[...].reshape(rows * head_count, width)
    own_logits = jnp.dot(query, latent[...], preferred_element_type=jnp.float32) * softmax_scale
    near_logits = jnp.dot(query, near_latent[...], preferred_element_type=jnp.float32) * softmax_scale
    slot = lax.broadcasted_iota(jnp.int32, (head_count, keys), 1)
    own_weights, near_weights = [], []
    for t in range(rows):
        position = qpos[2 * t + column]
        own_allowed = slot < jnp.minimum(valid[0], position - me * keys + 1)
        near_allowed = slot < jnp.minimum(near_valid[0], position - partner * keys + 1)
        of = slice(t * head_count, (t + 1) * head_count)
        own_scores = jnp.where(own_allowed, own_logits[of], MASKED)
        near_scores = jnp.where(near_allowed, near_logits[of], MASKED)
        top = jnp.max(jnp.maximum(own_scores, near_scores), axis=1, keepdims=True)
        own_weight = jnp.where(own_allowed, jnp.exp(own_scores - top), 0.0)
        near_weight = jnp.where(near_allowed, jnp.exp(near_scores - top), 0.0)
        stat_m[of, :] = jnp.broadcast_to(top, (head_count, LANES))
        stat_l[of, :] = jnp.broadcast_to(
            jnp.sum(own_weight + near_weight, axis=1, keepdims=True), (head_count, LANES)
        )
        own_weights.append(own_weight.astype(jnp.bfloat16))
        near_weights.append(near_weight.astype(jnp.bfloat16))
    transposed = (((1,), (1,)), ((), ()))
    mixed_all = lax.dot_general(
        jnp.concatenate(own_weights, axis=0),
        latent[:nope, :],
        transposed,
        preferred_element_type=jnp.float32,
    ) + lax.dot_general(
        jnp.concatenate(near_weights, axis=0),
        near_latent[:nope, :],
        transposed,
        preferred_element_type=jnp.float32,
    )
    for c in range(mix.shape[0]):
        mix[c] = mixed_all[:, c * LANES : (c + 1) * LANES]

    tile_lane = lax.broadcasted_iota(jnp.int32, (lines, LANES), 1)
    even = lax.rem(lax.broadcasted_iota(jnp.int32, (lines, LANES), 0), 2) == 0
    moved = []
    for k in range(rows - 1, -1, -1):
        group = flip(row, k)
        stat = jnp.zeros((lines, LANES), jnp.float32)
        for j in range(per):
            of = pl.ds(group * per + j, lines, stride=twin)
            stat = jnp.where(tile_lane == j, stat_m[of, :], stat)
            stat = jnp.where(tile_lane == per + j, stat_l[of, :], stat)
        st_send[k] = stat
        if k:
            moved.append(
                remote(st_send.at[k], st_recv.at[k], st_ssem.at[k], st_rsem.at[k], ctx=flip(me, 2 * k))
            )
    for copy in up_in:
        copy.wait()
    for k in range(rows - 1, -1, -1):
        group = flip(row, k)
        for j in range(per):
            h = group * per + j
            of = pl.ds(h, lines, stride=twin)
            mixed = jnp.concatenate(
                [mix[c, of, :] for c in range(mix.shape[0])], axis=1
            ).astype(jnp.bfloat16)
            num_send[k, j] = jnp.where(
                even,
                jnp.dot(mixed, up[h], preferred_element_type=jnp.float32),
                jnp.dot(mixed, up[h + twin], preferred_element_type=jnp.float32),
            ).astype(jnp.bfloat16)
        if k:
            moved.append(
                remote(num_send.at[k], num_recv.at[k], num_ssem.at[k], num_rsem.at[k], ctx=flip(me, 2 * k))
            )
    for copy in moved:
        copy.wait_recv()

    stats = [st_send[0]] + [st_recv[k] for k in range(1, rows)]
    top = functools.reduce(jnp.maximum, stats)
    factors = [jnp.exp(s - top) for s in stats]
    for j in range(per):
        total = jnp.zeros((lines, 1), jnp.float32)
        value = jnp.zeros((lines, vhead), jnp.float32)
        for k, (s, f) in enumerate(zip(stats, factors)):
            factor = f[:, j : j + 1]
            total += factor * s[:, per + j : per + j + 1]
            value += factor * (num_recv if k else num_send)[k, j].astype(jnp.float32)
        att_all[row, column, j] = (value / total).astype(jnp.bfloat16)

    shared = {}
    for k in range(n - 1, 0, -1):
        if k % 2 and k > 1:
            admit(k)
        shared[k] = remote(
            att_all.at[row, column],
            att_all.at[row, column],
            att_ssem.at[k],
            att_rsem.at[k],
            ctx=flip(me, k),
        )
    for copy in near + queries + relayed + moved:
        copy.wait_send()
    for copy in out_in:
        copy.wait()
    columns = outw.shape[1]
    acc = jnp.zeros((2 * lines, columns), jnp.float32)
    both = lax.rem(lax.broadcasted_iota(jnp.int32, (2 * lines, LANES), 0), 2) == 0
    own_line = lax.broadcasted_iota(jnp.int32, (lines, LANES), 0)

    def keep(group):
        for j in range(per):
            tile = att_all[group, column, j].astype(jnp.float32)
            for p in range(2):
                at = pl.multiple_of((p * twin + group * per + j) * vhead, vhead)
                attn_ref[:, pl.ds(at, vhead)] = jnp.sum(
                    jnp.where(own_line == 2 * row + p, tile, 0.0), axis=0, keepdims=True
                )

    for k in range(rows):
        group = flip(row, k)
        if k:
            shared[2 * k].wait_recv()
        shared[2 * k + 1].wait_recv()
        evens, odds = [], []
        for j in range(per):
            tile = jnp.concatenate(
                [att_all[group, c, j].astype(jnp.float32) for c in range(2)], axis=0
            )
            evens.append(jnp.where(both, tile, 0.0).astype(jnp.bfloat16))
            odds.append(jnp.where(both, 0.0, tile).astype(jnp.bfloat16))
        for p, side in enumerate((evens, odds)):
            at = pl.multiple_of((p * twin + group * per) * vhead, per * vhead)
            acc += jnp.dot(
                jnp.concatenate(side, axis=1),
                outw[pl.ds(at, per * vhead), :],
                preferred_element_type=jnp.float32,
            )
        if k < rows - 1:
            keep(group)
    share = n // heads
    for i in range(heads):
        lots = []
        for token in range(i * share, (i + 1) * share):
            at = token % 2 * lines + token // 2 * 2
            lots.append(acc[at : at + 1] + acc[at + 1 : at + 2])
        part[i] = jnp.concatenate(lots, axis=0)
    swap = remote(part.at[other], part_recv, part_ssem.at[0], part_rsem.at[0], head=other)
    keep(flip(row, rows - 1))
    swap.wait_recv()
    proj_ref[...] = part[hd] + part_recv[...]
    for k in range(n - 1, 0, -1):
        shared[k].wait_send()
    swap.wait_send()


def finish(attn_ref, summed_ref, scales_ref, attn_out, proj_out):
    attn_out[...] = attn_ref[...].astype(jnp.bfloat16)
    proj_out[...] = (summed_ref[...] * scales_ref[...].reshape(1, -1)).astype(jnp.bfloat16)


def block(n, heads, *args):
    query, codes, scales, valid, qpos, up, outw, out_scales = args
    own, head_count, width = query.shape
    keys, blocks = scales.shape
    split = 3 * heads
    fits = own == 1 and heads == 2 and n >= 4 and n & (n - 1) == 0 and head_count % n == 0
    fits = fits and width % (split * 16) == 0
    if not fits:
        return shards(*args)
    vhead = up.shape[2]
    rows, lines = n // 2, n
    per = head_count // n
    columns = outw.shape[1]
    anywhere = pl.BlockSpec(memory_space=pltpu.HBM)
    vmem = pl.BlockSpec(memory_space=pltpu.VMEM)
    dma = pltpu.SemaphoreType.DMA
    attention, summed = pl.pallas_call(
        functools.partial(fused, n, heads),
        out_shape=(
            jax.ShapeDtypeStruct((own, head_count * vhead), jnp.float32),
            jax.ShapeDtypeStruct((n // heads, columns), jnp.float32),
        ),
        in_specs=[anywhere] * 7,
        out_specs=(vmem, vmem),
        scratch_shapes=[
            pltpu.SMEM(valid.shape, jnp.int32),
            pltpu.SMEM(qpos.shape, jnp.int32),
            pltpu.SMEM(valid.shape, jnp.int32),
            pltpu.VMEM((rows, head_count, width), jnp.bfloat16),
            pltpu.VMEM((split, width // split, keys), jnp.bfloat16),
            pltpu.VMEM((split, width // split, keys), jnp.bfloat16),
            pltpu.VMEM((blocks, keys), jnp.float32),
            pltpu.VMEM((blocks, keys), jnp.float32),
            pltpu.VMEM(up.shape, jnp.bfloat16),
            pltpu.VMEM(outw.shape, jnp.bfloat16),
            pltpu.VMEM((width, keys), jnp.bfloat16),
            pltpu.VMEM((width, keys), jnp.bfloat16),
            pltpu.VMEM((LAT_NOPE // LANES, rows * head_count, LANES), jnp.float32),
            pltpu.VMEM((rows * head_count, LANES), jnp.float32),
            pltpu.VMEM((rows * head_count, LANES), jnp.float32),
            pltpu.VMEM((rows, per, lines, vhead), jnp.bfloat16),
            pltpu.VMEM((rows, per, lines, vhead), jnp.bfloat16),
            pltpu.VMEM((rows, lines, LANES), jnp.float32),
            pltpu.VMEM((rows, lines, LANES), jnp.float32),
            pltpu.VMEM((rows, 2, per, lines, vhead), jnp.bfloat16),
            pltpu.VMEM((heads, n // heads, columns), jnp.float32),
            pltpu.VMEM((n // heads, columns), jnp.float32),
            pltpu.SemaphoreType.REGULAR((n,)),
            dma((5,)),
            dma((2,)),
            dma((2,)),
            dma((rows,)),
            dma((rows,)),
            dma((split // heads + 2,)),
            dma((split // heads + 2,)),
            dma((split // heads,)),
            dma((split // heads,)),
            dma((rows,)),
            dma((rows,)),
            dma((rows,)),
            dma((rows,)),
            dma((n,)),
            dma((n,)),
            dma((1,)),
            dma((1,)),
        ],
        compiler_params=pltpu.CompilerParams(
            collective_id=0, has_side_effects=True
        ),
        name="mla_block",
    )(
        valid,
        qpos,
        query,
        codes.T.reshape(split, width // split, keys),
        scales.T,
        up,
        outw,
    )
    return pl.pallas_call(
        finish,
        out_shape=(
            jax.ShapeDtypeStruct((own, head_count * vhead), jnp.bfloat16),
            jax.ShapeDtypeStruct((n // heads, columns), jnp.bfloat16),
        ),
        in_specs=[vmem] * 3,
        out_specs=(vmem, vmem),
        name="finish",
    )(attention, summed, out_scales)


def solution(mesh):
    ctx, heads = mesh.shape["ctx"], mesh.shape["head"]
    return jax.shard_map(
        functools.partial(block, ctx, heads),
        mesh=mesh,
        in_specs=(
            P(("groups", "ctx"), "head", None),
            P(("groups", "ctx"), None),
            P(("groups", "ctx"), None),
            P(("groups", "ctx")),
            P("groups"),
            P("head", None, None),
            P("head", "ctx"),
            P("ctx"),
        ),
        out_specs=(P(("groups", "ctx"), "head"), P(("groups", "head"), "ctx")),
        check_vma=False,
    )
```

```python
import functools
import math

import jax
import jax.numpy as jnp
from jax import lax
from jax.experimental import pallas as pl
from jax.experimental.pallas import tpu as pltpu
from jax.sharding import PartitionSpec as P

LAT_NOPE = 512
ROPE = 64
QK_NOPE = 128
LANES = 128
MASKED = -1e30
MESH = pl.DeviceIdType.MESH


def shards(
    query_latent,
    latent_codes,
    latent_scales,
    valid_lengths,
    query_position,
    value_up,
    out_codes,
    out_scales,
):
    key_count, width = latent_codes.shape
    block_count = latent_scales.shape[1]
    latent = (
        (
            latent_codes.astype(jnp.float32).reshape(key_count, block_count, width // block_count)
            * latent_scales[:, :, None]
        )
        .reshape(key_count, width)
        .astype(jnp.bfloat16)
    )
    shard_index = lax.axis_index("ctx")
    local_slots = jnp.arange(key_count, dtype=jnp.int32)
    key_pos = shard_index * key_count + local_slots
    usable = local_slots < valid_lengths[0]
    softmax_scale = (QK_NOPE + ROPE) ** (-0.5)
    logits = (
        jnp.einsum(
            "qhc,kc->qhk",
            lax.all_gather(query_latent, "ctx", axis=0, tiled=True),
            latent,
            preferred_element_type=jnp.float32,
        )
        * softmax_scale
    )
    allowed = usable[None, :] & (key_pos[None, :] <= query_position[:, None])
    scores = jnp.where(allowed[:, None, :], logits, -jnp.inf)
    maxima = lax.pmax(jnp.max(scores, axis=2), "ctx")
    weights = jnp.exp(scores - maxima[:, :, None])
    totals = jnp.sum(weights, axis=2)
    latent_mix = jnp.einsum(
        "qhk,kd->qhd",
        weights.astype(jnp.bfloat16),
        latent[:, :LAT_NOPE],
        preferred_element_type=jnp.float32,
    ).astype(jnp.bfloat16)
    values = jnp.einsum("qhd,hdv->qhv", latent_mix, value_up, preferred_element_type=jnp.float32)
    queries, head_count, value_width = values.shape
    numerators = values.reshape(queries, head_count * value_width)
    own_rows = query_latent.shape[0]
    numer_sum, denom_sum = lax.psum((numerators, totals), "ctx")
    attn_all = (
        (numer_sum.reshape(queries, head_count, value_width) / denom_sum[:, :, None])
        .reshape(queries, head_count * value_width)
        .astype(jnp.bfloat16)
    )
    attn_home = lax.dynamic_slice_in_dim(attn_all, shard_index * own_rows, own_rows, 0)
    summed = lax.psum_scatter(
        jnp.dot(attn_all, out_codes, preferred_element_type=jnp.float32),
        "head",
        scatter_dimension=0,
        tiled=True,
    )
    projected = (summed * out_scales[None, :]).astype(jnp.bfloat16)
    return (attn_home, projected)


def flip(index, mask):
    bit, result = 1, index
    while bit <= mask:
        if mask & bit:
            result = result + bit - 2 * bit * lax.rem(index // bit, 2)
        bit *= 2
    return result


def fused(
    n,
    heads,
    valid_hbm,
    qpos_hbm,
    query_hbm,
    codes_hbm,
    scales_hbm,
    up_hbm,
    out_hbm,
    attn_ref,
    proj_ref,
    valid,
    qpos,
    near_valid,
    q_all,
    codes,
    near_codes,
    scales,
    near_scales,
    up,
    outw,
    latent,
    near_latent,
    mix,
    stat_m,
    stat_l,
    num_send,
    num_recv,
    st_send,
    st_recv,
    att_all,
    part,
    part_recv,
    ready,
    in_sem,
    up_sem,
    out_sem,
    q_ssem,
    q_rsem,
    near_ssem,
    near_rsem,
    half_ssem,
    half_rsem,
    num_ssem,
    num_rsem,
    st_ssem,
    st_rsem,
    att_ssem,
    att_rsem,
    part_ssem,
    part_rsem,
):
    me = lax.axis_index("ctx")
    hd = lax.axis_index("head")
    other = 1 - hd
    row, column = me // 2, lax.rem(me, 2)
    rows = n // 2
    head_count, width = q_all.shape[1:]
    blocks, block, keys = codes.shape
    pairs = (blocks - 1) // 2
    rest = pl.ds(2 * pairs, blocks - 2 * pairs)
    nope = mix.shape[0] * LANES
    vhead = up.shape[2]
    twin = head_count // 2
    per = twin // rows
    lines = 2 * rows

    barrier = pltpu.get_barrier_semaphore()
    met = [1] + list(range(2, n, 2))
    for k in met:
        later = flip(me, k)

        @pl.when(later > me)
        def _():
            pl.semaphore_signal(barrier, inc=1, device_id={"ctx": later}, device_id_type=MESH)

    @pl.when(hd == 0)
    def _():
        pl.semaphore_signal(barrier, inc=1, device_id={"head": other}, device_id_type=MESH)

    loads = [
        pltpu.make_async_copy(codes_hbm, codes, in_sem.at[0]),
        pltpu.make_async_copy(scales_hbm, scales, in_sem.at[1]),
        pltpu.make_async_copy(query_hbm.at[0], q_all.at[row], in_sem.at[2]),
        pltpu.make_async_copy(valid_hbm, valid, in_sem.at[3]),
        pltpu.make_async_copy(qpos_hbm, qpos, in_sem.at[4]),
    ]
    for copy in loads:
        copy.start()

    ahead = row + column + hd

    @pl.when(ahead > 0)
    def _():
        pl.semaphore_wait(barrier, ahead)

    @pl.when(hd == 1)
    def _():
        pl.semaphore_signal(ready.at[0], inc=1, device_id={"head": other}, device_id_type=MESH)

    for k in met:
        earlier = flip(me, k)

        @pl.when(earlier < me)
        def _():
            pl.semaphore_signal(ready.at[k], inc=1, device_id={"ctx": earlier}, device_id_type=MESH)

    def admit(k):
        @pl.when(flip(me, k) > me)
        def _():
            pl.semaphore_wait(ready.at[k], 1)

    def owner(p):
        return int(p >= 1)

    def remote(src, dst, ssem, rsem, when=None, **device):
        copy = pltpu.make_async_remote_copy(
            src_ref=src,
            dst_ref=dst,
            send_sem=ssem,
            recv_sem=rsem,
            device_id=device,
            device_id_type=MESH,
        )
        copy.start() if when is None else pl.when(when)(copy.start)
        return copy

    queries = []
    for k in range(1, rows):
        peer = flip(me, 2 * k)
        queries.append(remote(query_hbm.at[0], q_all.at[row], q_ssem.at[k], q_rsem.at[k], peer < me, ctx=peer))

    admit(1)
    partner = flip(me, 1)
    near = [
        remote(valid_hbm, near_valid, near_ssem.at[0], near_rsem.at[0], ctx=partner),
        remote(scales_hbm, near_scales, near_ssem.at[1], near_rsem.at[1], hd == 1, ctx=partner),
    ]
    for p in range(pairs):
        of = pl.ds(2 * p, 2)
        near.append(
            remote(
                codes_hbm.at[of],
                near_codes.at[of],
                near_ssem.at[2 + p],
                near_rsem.at[2 + p],
                hd == owner(p),
                ctx=partner,
            )
        )
    last = remote(
        codes_hbm.at[rest],
        near_codes.at[rest],
        near_ssem.at[2 + pairs],
        near_rsem.at[2 + pairs],
        ctx=partner,
    )

    up_in = []
    for g in range(2):
        part_of = pl.ds(g * twin, twin)
        up_in.append(pltpu.make_async_copy(up_hbm.at[part_of], up.at[part_of], up_sem.at[g]))
        up_in[-1].start()
    for k in range(1, rows):
        admit(2 * k)
        pl.when(flip(me, 2 * k) > me)(queries[k - 1].start)

    out_in = []
    half = outw.shape[0] // 2
    for g in range(2):
        part_of = pl.ds(g * half, half)
        out_in.append(pltpu.make_async_copy(out_hbm.at[part_of], outw.at[part_of], out_sem.at[g]))
        out_in[-1].start()
    def scale_latent(source, factors, target, of):
        for b in of:
            target[b * block : (b + 1) * block, :] = (
                source[b].astype(jnp.float32) * factors[b : b + 1, :]
            ).astype(jnp.bfloat16)

    for copy in loads:
        copy.wait()
    scale_latent(codes, scales, latent, range(blocks))

    relayed = []

    def relay(ref, index, who):
        pl.when(hd == who)(near[index].wait_recv)
        relayed.append(
            remote(ref, ref, half_ssem.at[index], half_rsem.at[index], hd == who, head=other)
        )

    @pl.when(hd == 0)
    def _():
        pl.semaphore_wait(ready.at[0], 1)

    relay(near_scales, 1, 1)
    for p in range(pairs):
        relay(near_codes.at[pl.ds(2 * p, 2)], 2 + p, owner(p))
    for copy in queries:
        copy.wait_recv()
    softmax_scale = (QK_NOPE + ROPE) ** (-0.5)
    query = q_all[...].reshape(rows * head_count, width)
    own_logits = jnp.dot(query, latent[...], preferred_element_type=jnp.float32) * softmax_scale
    pl.when(hd == 0)(relayed[0].wait_recv)
    near[0].wait_recv()
    near_logits = None
    for p in list(range(pairs - 1)) + [pairs, pairs - 1]:
        if p < pairs:
            pl.when(hd != owner(p))(relayed[1 + p].wait_recv)
        else:
            last.wait_recv()
        of = range(2 * p, min(2 * p + 2, blocks))
        scale_latent(near_codes, near_scales, near_latent, of)
        lanes = slice(of[0] * block, (of[-1] + 1) * block)
        term = jnp.dot(query[:, lanes], near_latent[lanes, :], preferred_element_type=jnp.float32)
        near_logits = term if near_logits is None else near_logits + term
    near_logits = near_logits * softmax_scale
    slot = lax.broadcasted_iota(jnp.int32, (head_count, keys), 1)
    own_weights, near_weights = [], []
    for t in range(rows):
        position = qpos[2 * t + column]
        own_allowed = slot < jnp.minimum(valid[0], position - me * keys + 1)
        near_allowed = slot < jnp.minimum(near_valid[0], position - partner * keys + 1)
        of = slice(t * head_count, (t + 1) * head_count)
        own_scores = jnp.where(own_allowed, own_logits[of], MASKED)
        near_scores = jnp.where(near_allowed, near_logits[of], MASKED)
        top = jnp.max(jnp.maximum(own_scores, near_scores), axis=1, keepdims=True)
        own_weight = jnp.where(own_allowed, jnp.exp(own_scores - top), 0.0)
        near_weight = jnp.where(near_allowed, jnp.exp(near_scores - top), 0.0)
        stat_m[of, :] = jnp.broadcast_to(top, (head_count, LANES))
        stat_l[of, :] = jnp.broadcast_to(
            jnp.sum(own_weight + near_weight, axis=1, keepdims=True), (head_count, LANES)
        )
        own_weights.append(own_weight.astype(jnp.bfloat16))
        near_weights.append(near_weight.astype(jnp.bfloat16))
    transposed = (((1,), (1,)), ((), ()))
    mixed_all = lax.dot_general(
        jnp.concatenate(own_weights, axis=0),
        latent[:nope, :],
        transposed,
        preferred_element_type=jnp.float32,
    ) + lax.dot_general(
        jnp.concatenate(near_weights, axis=0),
        near_latent[:nope, :],
        transposed,
        preferred_element_type=jnp.float32,
    )
    for c in range(mix.shape[0]):
        mix[c] = mixed_all[:, c * LANES : (c + 1) * LANES]

    tile_lane = lax.broadcasted_iota(jnp.int32, (lines, LANES), 1)
    even = lax.rem(lax.broadcasted_iota(jnp.int32, (lines, LANES), 0), 2) == 0
    moved = []
    for k in range(rows - 1, -1, -1):
        group = flip(row, k)
        stat = jnp.zeros((lines, LANES), jnp.float32)
        for j in range(per):
            of = pl.ds(group * per + j, lines, stride=twin)
            stat = jnp.where(tile_lane == j, stat_m[of, :], stat)
            stat = jnp.where(tile_lane == per + j, stat_l[of, :], stat)
        st_send[k] = stat
        if k:
            moved.append(
                remote(st_send.at[k], st_recv.at[k], st_ssem.at[k], st_rsem.at[k], ctx=flip(me, 2 * k))
            )
    for copy in up_in:
        copy.wait()
    for k in range(rows - 1, -1, -1):
        group = flip(row, k)
        for j in range(per):
            h = group * per + j
            of = pl.ds(h, lines, stride=twin)
            mixed = jnp.concatenate(
                [mix[c, of, :] for c in range(mix.shape[0])], axis=1
            ).astype(jnp.bfloat16)
            num_send[k, j] = jnp.where(
                even,
                jnp.dot(mixed, up[h], preferred_element_type=jnp.float32),
                jnp.dot(mixed, up[h + twin], preferred_element_type=jnp.float32),
            ).astype(jnp.bfloat16)
        if k:
            moved.append(
                remote(num_send.at[k], num_recv.at[k], num_ssem.at[k], num_rsem.at[k], ctx=flip(me, 2 * k))
            )
    for copy in moved:
        copy.wait_recv()

    stats = [st_send[0]] + [st_recv[k] for k in range(1, rows)]
    top = functools.reduce(jnp.maximum, stats)
    factors = [jnp.exp(s - top) for s in stats]
    for j in range(per):
        total = jnp.zeros((lines, 1), jnp.float32)
        value = jnp.zeros((lines, vhead), jnp.float32)
        for k, (s, f) in enumerate(zip(stats, factors)):
            factor = f[:, j : j + 1]
            total += factor * s[:, per + j : per + j + 1]
            value += factor * (num_recv if k else num_send)[k, j].astype(jnp.float32)
        att_all[row, column, j] = (value / total).astype(jnp.bfloat16)

    shared = {}
    for k in range(n - 1, 0, -1):
        shared[k] = remote(
            att_all.at[row, column],
            att_all.at[row, column],
            att_ssem.at[k],
            att_rsem.at[k],
            ctx=flip(me, k),
        )
    for copy in [near[0], last] + queries + moved:
        copy.wait_send()
    for p in range(-1, pairs):
        pl.when(hd == (owner(p) if p >= 0 else 1))(near[2 + p].wait_send)
        pl.when(hd == (owner(p) if p >= 0 else 1))(relayed[1 + p].wait_send)
    for copy in out_in:
        copy.wait()
    columns = outw.shape[1]
    acc = jnp.zeros((2 * lines, columns), jnp.float32)
    both = lax.rem(lax.broadcasted_iota(jnp.int32, (2 * lines, LANES), 0), 2) == 0
    own_line = lax.broadcasted_iota(jnp.int32, (lines, LANES), 0)

    def keep(group):
        for j in range(per):
            tile = att_all[group, column, j].astype(jnp.float32)
            for p in range(2):
                at = pl.multiple_of((p * twin + group * per + j) * vhead, vhead)
                attn_ref[:, pl.ds(at, vhead)] = jnp.sum(
                    jnp.where(own_line == 2 * row + p, tile, 0.0), axis=0, keepdims=True
                )

    for k in range(rows):
        group = flip(row, k)
        if k:
            shared[2 * k].wait_recv()
        shared[2 * k + 1].wait_recv()
        evens, odds = [], []
        for j in range(per):
            tile = jnp.concatenate(
                [att_all[group, c, j].astype(jnp.float32) for c in range(2)], axis=0
            )
            evens.append(jnp.where(both, tile, 0.0).astype(jnp.bfloat16))
            odds.append(jnp.where(both, 0.0, tile).astype(jnp.bfloat16))
        for p, side in enumerate((evens, odds)):
            at = pl.multiple_of((p * twin + group * per) * vhead, per * vhead)
            acc += jnp.dot(
                jnp.concatenate(side, axis=1),
                outw[pl.ds(at, per * vhead), :],
                preferred_element_type=jnp.float32,
            )
        if k < rows - 1:
            keep(group)
    share = n // heads
    for i in range(heads):
        lots = []
        for token in range(i * share, (i + 1) * share):
            at = token % 2 * lines + token // 2 * 2
            lots.append(acc[at : at + 1] + acc[at + 1 : at + 2])
        part[i] = jnp.concatenate(lots, axis=0)
    swap = remote(part.at[other], part_recv, part_ssem.at[0], part_rsem.at[0], head=other)
    keep(flip(row, rows - 1))
    swap.wait_recv()
    proj_ref[...] = part[hd] + part_recv[...]
    for k in range(n - 1, 0, -1):
        shared[k].wait_send()
    swap.wait_send()


def finish(attn_ref, summed_ref, scales_ref, attn_out, proj_out):
    attn_out[...] = attn_ref[...].astype(jnp.bfloat16)
    proj_out[...] = (summed_ref[...] * scales_ref[...].reshape(1, -1)).astype(jnp.bfloat16)


def block(n, heads, *args):
    query, codes, scales, valid, qpos, up, outw, out_scales = args
    own, head_count, width = query.shape
    keys, blocks = scales.shape
    chunk = (blocks - 1) // 2 + 3
    fits = own == 1 and heads == 2 and n >= 4 and n & (n - 1) == 0 and head_count % n == 0
    fits = fits and width % blocks == 0 and 2 * width // blocks % LANES == 0 and blocks > 2
    if not fits:
        return shards(*args)
    vhead = up.shape[2]
    rows, lines = n // 2, n
    per = head_count // n
    columns = outw.shape[1]
    anywhere = pl.BlockSpec(memory_space=pltpu.HBM)
    vmem = pl.BlockSpec(memory_space=pltpu.VMEM)
    dma = pltpu.SemaphoreType.DMA
    attention, summed = pl.pallas_call(
        functools.partial(fused, n, heads),
        out_shape=(
            jax.ShapeDtypeStruct((own, head_count * vhead), jnp.float32),
            jax.ShapeDtypeStruct((n // heads, columns), jnp.float32),
        ),
        in_specs=[anywhere] * 7,
        out_specs=(vmem, vmem),
        scratch_shapes=[
            pltpu.SMEM(valid.shape, jnp.int32),
            pltpu.SMEM(qpos.shape, jnp.int32),
            pltpu.SMEM(valid.shape, jnp.int32),
            pltpu.VMEM((rows, head_count, width), jnp.bfloat16),
            pltpu.VMEM((blocks, width // blocks, keys), jnp.bfloat16),
            pltpu.VMEM((blocks, width // blocks, keys), jnp.bfloat16),
            pltpu.VMEM((blocks, keys), jnp.float32),
            pltpu.VMEM((blocks, keys), jnp.float32),
            pltpu.VMEM(up.shape, jnp.bfloat16),
            pltpu.VMEM(outw.shape, jnp.bfloat16),
            pltpu.VMEM((width, keys), jnp.bfloat16),
            pltpu.VMEM((width, keys), jnp.bfloat16),
            pltpu.VMEM((LAT_NOPE // LANES, rows * head_count, LANES), jnp.float32),
            pltpu.VMEM((rows * head_count, LANES), jnp.float32),
            pltpu.VMEM((rows * head_count, LANES), jnp.float32),
            pltpu.VMEM((rows, per, lines, vhead), jnp.bfloat16),
            pltpu.VMEM((rows, per, lines, vhead), jnp.bfloat16),
            pltpu.VMEM((rows, lines, LANES), jnp.float32),
            pltpu.VMEM((rows, lines, LANES), jnp.float32),
            pltpu.VMEM((rows, 2, per, lines, vhead), jnp.bfloat16),
            pltpu.VMEM((heads, n // heads, columns), jnp.float32),
            pltpu.VMEM((n // heads, columns), jnp.float32),
            pltpu.SemaphoreType.REGULAR((n,)),
            dma((5,)),
            dma((2,)),
            dma((2,)),
            dma((rows,)),
            dma((rows,)),
            dma((chunk,)),
            dma((chunk,)),
            dma((chunk,)),
            dma((chunk,)),
            dma((rows,)),
            dma((rows,)),
            dma((rows,)),
            dma((rows,)),
            dma((n,)),
            dma((n,)),
            dma((1,)),
            dma((1,)),
        ],
        compiler_params=pltpu.CompilerParams(
            collective_id=0, has_side_effects=True, vmem_limit_bytes=32 * 1024 * 1024
        ),
        name="mla_block",
    )(
        valid,
        *(
            pltpu.with_memory_space_constraint(operand, pltpu.HBM)
            for operand in (
                qpos,
                query,
                codes.T.reshape(blocks, width // blocks, keys),
                scales.T,
                up,
                outw,
            )
        ),
    )
    return pl.pallas_call(
        finish,
        out_shape=(
            jax.ShapeDtypeStruct((own, head_count * vhead), jnp.bfloat16),
            jax.ShapeDtypeStruct((n // heads, columns), jnp.bfloat16),
        ),
        in_specs=[vmem] * 3,
        out_specs=(vmem, vmem),
        compiler_params=pltpu.CompilerParams(vmem_limit_bytes=1024 * 1024),
        name="finish",
    )(attention, summed, out_scales)


def solution(mesh):
    ctx, heads = mesh.shape["ctx"], mesh.shape["head"]
    return jax.shard_map(
        functools.partial(block, ctx, heads),
        mesh=mesh,
        in_specs=(
            P(("groups", "ctx"), "head", None),
            P(("groups", "ctx"), None),
            P(("groups", "ctx"), None),
            P(("groups", "ctx")),
            P("groups"),
            P("head", None, None),
            P("head", "ctx"),
            P("ctx"),
        ),
        out_specs=(P(("groups", "ctx"), "head"), P(("groups", "head"), "ctx")),
        check_vma=False,
    )
```

```python
import functools
import math

import jax
import jax.numpy as jnp
from jax import lax
from jax.experimental import pallas as pl
from jax.experimental.pallas import tpu as pltpu
from jax.sharding import PartitionSpec as P

LAT_NOPE = 512
ROPE = 64
QK_NOPE = 128
LANES = 128
MASKED = -1e30
FLOOR = -1e29
EXPONENT = math.log2(math.e) * (QK_NOPE + ROPE) ** -0.5
MESH = pl.DeviceIdType.MESH


def shards(
    query_latent,
    latent_codes,
    latent_scales,
    valid_lengths,
    query_position,
    value_up,
    out_codes,
    out_scales,
):
    key_count, width = latent_codes.shape
    block_count = latent_scales.shape[1]
    latent = (
        (
            latent_codes.astype(jnp.float32).reshape(key_count, block_count, width // block_count)
            * latent_scales[:, :, None]
        )
        .reshape(key_count, width)
        .astype(jnp.bfloat16)
    )
    shard_index = lax.axis_index("ctx")
    local_slots = jnp.arange(key_count, dtype=jnp.int32)
    key_pos = shard_index * key_count + local_slots
    usable = local_slots < valid_lengths[0]
    softmax_scale = (QK_NOPE + ROPE) ** (-0.5)
    logits = (
        jnp.einsum(
            "qhc,kc->qhk",
            lax.all_gather(query_latent, "ctx", axis=0, tiled=True),
            latent,
            preferred_element_type=jnp.float32,
        )
        * softmax_scale
    )
    allowed = usable[None, :] & (key_pos[None, :] <= query_position[:, None])
    scores = jnp.where(allowed[:, None, :], logits, -jnp.inf)
    maxima = lax.pmax(jnp.max(scores, axis=2), "ctx")
    weights = jnp.exp(scores - maxima[:, :, None])
    totals = jnp.sum(weights, axis=2)
    latent_mix = jnp.einsum(
        "qhk,kd->qhd",
        weights.astype(jnp.bfloat16),
        latent[:, :LAT_NOPE],
        preferred_element_type=jnp.float32,
    ).astype(jnp.bfloat16)
    values = jnp.einsum("qhd,hdv->qhv", latent_mix, value_up, preferred_element_type=jnp.float32)
    queries, head_count, value_width = values.shape
    numerators = values.reshape(queries, head_count * value_width)
    own_rows = query_latent.shape[0]
    numer_sum, denom_sum = lax.psum((numerators, totals), "ctx")
    attn_all = (
        (numer_sum.reshape(queries, head_count, value_width) / denom_sum[:, :, None])
        .reshape(queries, head_count * value_width)
        .astype(jnp.bfloat16)
    )
    attn_home = lax.dynamic_slice_in_dim(attn_all, shard_index * own_rows, own_rows, 0)
    summed = lax.psum_scatter(
        jnp.dot(attn_all, out_codes, preferred_element_type=jnp.float32),
        "head",
        scatter_dimension=0,
        tiled=True,
    )
    projected = (summed * out_scales[None, :]).astype(jnp.bfloat16)
    return (attn_home, projected)


def flip(index, mask):
    bit, result = 1, index
    while bit <= mask:
        if mask & bit:
            result = result + bit - 2 * bit * lax.rem(index // bit, 2)
        bit *= 2
    return result


def fused(
    n,
    heads,
    valid_hbm,
    qpos_hbm,
    query_hbm,
    codes_hbm,
    scales_hbm,
    up_hbm,
    out_hbm,
    attn_ref,
    proj_ref,
    valid,
    qpos,
    near_valid,
    q_all,
    codes,
    near_codes,
    scales,
    near_scales,
    up,
    outw,
    latent,
    mix,
    stat_m,
    stat_l,
    num_send,
    num_recv,
    st_send,
    st_recv,
    att_all,
    part,
    part_recv,
    ready,
    in_sem,
    up_sem,
    out_sem,
    q_ssem,
    q_rsem,
    near_ssem,
    near_rsem,
    half_ssem,
    half_rsem,
    num_ssem,
    num_rsem,
    st_ssem,
    st_rsem,
    att_ssem,
    att_rsem,
    part_ssem,
    part_rsem,
):
    me = lax.axis_index("ctx")
    hd = lax.axis_index("head")
    other = 1 - hd
    row, column = me // 2, lax.rem(me, 2)
    rows = n // 2
    head_count, width = q_all.shape[1:]
    blocks, block, keys = codes.shape
    first = 3 * (blocks - 1) // 8
    units = [(b, min(2, first - b), 0) for b in range(0, first, 2)]
    units += [(b, min(2, blocks - 1 - b), 1) for b in range(first, blocks - 1, 2)]
    rest = pl.ds(blocks - 1, 1)
    nope = mix.shape[0] * LANES
    vhead = up.shape[2]
    twin = head_count // 2
    per = twin // rows
    lines = 2 * rows

    barrier = pltpu.get_barrier_semaphore()
    met = [1] + list(range(2, n, 2))

    def slot_of(k):
        return k if k < 2 else k // 2 + 1

    for k in met:
        later = flip(me, k)

        @pl.when(later > me)
        def _():
            pl.semaphore_signal(barrier, inc=1, device_id={"ctx": later}, device_id_type=MESH)

    @pl.when(hd == 0)
    def _():
        pl.semaphore_signal(barrier, inc=1, device_id={"head": other}, device_id_type=MESH)

    loads = [
        pltpu.make_async_copy(codes_hbm, codes, in_sem.at[0]),
        pltpu.make_async_copy(scales_hbm, scales, in_sem.at[1]),
        pltpu.make_async_copy(query_hbm.at[0], q_all.at[row], in_sem.at[2]),
        pltpu.make_async_copy(valid_hbm, valid, in_sem.at[3]),
        pltpu.make_async_copy(qpos_hbm, qpos, in_sem.at[4]),
    ]
    for copy in loads:
        copy.start()

    ahead = row + column + hd

    @pl.when(ahead > 0)
    def _():
        pl.semaphore_wait(barrier, ahead)

    @pl.when(hd == 1)
    def _():
        pl.semaphore_signal(ready.at[0], inc=1, device_id={"head": other}, device_id_type=MESH)

    for k in met:
        earlier = flip(me, k)

        @pl.when(earlier < me)
        def _():
            pl.semaphore_signal(ready.at[slot_of(k)], inc=1, device_id={"ctx": earlier}, device_id_type=MESH)

    def admit(k):
        @pl.when(flip(me, k) > me)
        def _():
            pl.semaphore_wait(ready.at[slot_of(k)], 1)

    def drain(ref, sem):
        pltpu.make_async_copy(ref, ref, sem).wait()

    def remote(src, dst, ssem, rsem, when=None, **device):
        copy = pltpu.make_async_remote_copy(
            src_ref=src,
            dst_ref=dst,
            send_sem=ssem,
            recv_sem=rsem,
            device_id=device,
            device_id_type=MESH,
        )
        copy.start() if when is None else pl.when(when)(copy.start)
        return copy

    for k in range(1, rows):
        peer = flip(me, 2 * k)
        remote(query_hbm.at[0], q_all.at[row], q_ssem, q_rsem, peer < me, ctx=peer)

    admit(1)
    partner = flip(me, 1)
    near = [
        remote(valid_hbm, near_valid, near_ssem.at[0], near_rsem.at[0], ctx=partner),
        remote(scales_hbm, near_scales, near_ssem.at[1], near_rsem.at[1], hd == 1, ctx=partner),
    ]
    for p, (b, count, who) in enumerate(units):
        of = pl.ds(b, count)
        near.append(
            remote(
                codes_hbm.at[of],
                near_codes.at[of],
                near_ssem.at[2],
                near_rsem.at[2 + p],
                hd == who,
                ctx=partner,
            )
        )
    last = remote(
        codes_hbm.at[rest],
        near_codes.at[rest],
        near_ssem.at[3],
        near_rsem.at[2 + len(units)],
        ctx=partner,
    )

    up_in = pltpu.make_async_copy(up_hbm, up, up_sem)
    up_in.start()
    loads.pop(2).wait()
    for k in range(1, rows):
        admit(2 * k)
        peer = flip(me, 2 * k)
        remote(q_all.at[row], q_all.at[row], q_ssem, q_rsem, peer > me, ctx=peer)

    out_in = pltpu.make_async_copy(out_hbm, outw, out_sem)
    out_in.start()

    def scale_latent(source, factors, at, of):
        for b in of:
            latent[b * block : (b + 1) * block, at : at + keys] = (
                source[b].astype(jnp.float32) * factors[b : b + 1, :]
            ).astype(jnp.bfloat16)

    for copy in loads:
        copy.wait()
    scale_latent(codes, scales, 0, range(blocks))

    relayed = []

    def relay(ref, index, who):
        pl.when(hd == who)(near[index].wait_recv)
        relayed.append(
            remote(ref, ref, half_ssem.at[min(index, 2) - 1], half_rsem.at[index - 1], hd == who, head=other)
        )

    @pl.when(hd == 0)
    def _():
        pl.semaphore_wait(ready.at[0], 1)

    relay(near_scales, 1, 1)
    for p, (b, count, who) in enumerate(units):
        relay(near_codes.at[pl.ds(b, count)], 2 + p, who)
    pl.when(hd == 0)(relayed[0].wait_recv)
    near[0].wait_recv()
    for p, (b, count, who) in enumerate(units):
        pl.when(hd != who)(relayed[1 + p].wait_recv)
        scale_latent(near_codes, near_scales, keys, range(b, b + count))
    last.wait_recv()
    scale_latent(near_codes, near_scales, keys, range(blocks - 1, blocks))
    drain(q_all.at[pl.ds(0, rows - 1)], q_rsem)
    logits = jnp.dot(
        q_all[...].reshape(rows * head_count, width), latent[...], preferred_element_type=jnp.float32
    )
    slot = lax.broadcasted_iota(jnp.int32, (head_count, 2 * keys), 1)
    weights = []
    for t in range(rows):
        position = qpos[2 * t + column]
        own_limit = jnp.minimum(valid[0], position - me * keys + 1)
        near_limit = jnp.minimum(near_valid[0], position - partner * keys + 1)
        allowed = slot < jnp.where(slot < keys, own_limit, near_limit + keys)
        of = slice(t * head_count, (t + 1) * head_count)
        scores = jnp.where(allowed, logits[of], MASKED)
        top = jnp.maximum(jnp.max(scores, axis=1, keepdims=True), FLOOR)
        weight = jnp.exp2((scores - top) * EXPONENT)
        stat_m[of, :] = jnp.broadcast_to(top, (head_count, LANES))
        stat_l[of, :] = jnp.broadcast_to(jnp.sum(weight, axis=1, keepdims=True), (head_count, LANES))
        weights.append(weight.astype(jnp.bfloat16))
    mixed_all = lax.dot_general(
        jnp.concatenate(weights, axis=0),
        latent[:nope, :],
        (((1,), (1,)), ((), ())),
        preferred_element_type=jnp.float32,
    )
    for c in range(mix.shape[0]):
        mix[c] = mixed_all[:, c * LANES : (c + 1) * LANES]

    up_in.wait()
    tile_lane = lax.broadcasted_iota(jnp.int32, (lines, LANES), 1)
    even = lax.rem(lax.broadcasted_iota(jnp.int32, (lines, LANES), 0), 2) == 0
    for k in range(rows - 1, -1, -1):
        group = flip(row, k)
        stat = jnp.zeros((lines, LANES), jnp.float32)
        for j in range(per):
            of = pl.ds(group * per + j, lines, stride=twin)
            stat = jnp.where(tile_lane == j, stat_m[of, :], stat)
            stat = jnp.where(tile_lane == per + j, stat_l[of, :], stat)
        st_send[k] = stat
        if k:
            remote(st_send.at[k], st_recv.at[k], st_ssem, st_rsem, ctx=flip(me, 2 * k))
        for j in range(per):
            h = group * per + j
            of = pl.ds(h, lines, stride=twin)
            mixed = jnp.concatenate(
                [mix[c, of, :] for c in range(mix.shape[0])], axis=1
            ).astype(jnp.bfloat16)
            pair = jnp.dot(
                mixed,
                jnp.concatenate([up[h], up[h + twin]], axis=1),
                preferred_element_type=jnp.float32,
            )
            num_send[k, j] = jnp.where(even, pair[:, :vhead], pair[:, vhead:]).astype(jnp.bfloat16)
        if k:
            remote(num_send.at[k], num_recv.at[k], num_ssem, num_rsem, ctx=flip(me, 2 * k))
    drain(st_recv.at[pl.ds(1, rows - 1)], st_rsem)
    drain(num_recv.at[pl.ds(1, rows - 1)], num_rsem)

    stats = [st_send[0]] + [st_recv[k] for k in range(1, rows)]
    top = functools.reduce(jnp.maximum, stats)
    factors = [jnp.exp2((s - top) * EXPONENT) for s in stats]
    for j in range(per):
        total = jnp.zeros((lines, 1), jnp.float32)
        value = jnp.zeros((lines, vhead), jnp.float32)
        for k, (s, f) in enumerate(zip(stats, factors)):
            factor = f[:, j : j + 1]
            total += factor * s[:, per + j : per + j + 1]
            value += factor * (num_recv if k else num_send)[k, j].astype(jnp.float32)
        att_all[me, j] = (value / total).astype(jnp.bfloat16)

    for k in range(n - 1, 0, -1):
        remote(
            att_all.at[me],
            att_all.at[me],
            att_ssem,
            att_rsem.at[k // 2],
            ctx=flip(me, k),
        )
    for copy in [near[0], last]:
        copy.wait_send()
    drain(q_all.at[pl.ds(0, rows - 1)], q_ssem)
    drain(st_send.at[pl.ds(1, rows - 1)], st_ssem)
    drain(num_send.at[pl.ds(1, rows - 1)], num_ssem)

    @pl.when(hd == 0)
    def _():
        ours = near_codes.at[pl.ds(0, first)]
        drain(ours, near_ssem.at[2])
        drain(ours, half_ssem.at[1])

    @pl.when(hd == 1)
    def _():
        ours = near_codes.at[pl.ds(first, blocks - 1 - first)]
        drain(near_scales, near_ssem.at[1])
        drain(near_scales, half_ssem.at[0])
        drain(ours, near_ssem.at[2])
        drain(ours, half_ssem.at[1])

    out_in.wait()
    columns = outw.shape[1]
    acc = jnp.zeros((2 * lines, columns), jnp.float32)
    both = lax.rem(lax.broadcasted_iota(jnp.int32, (2 * lines, LANES), 0), 2) == 0
    own_line = lax.broadcasted_iota(jnp.int32, (lines, LANES), 0)

    def keep(group):
        for j in range(per):
            tile = att_all[2 * group + column, j].astype(jnp.float32)
            for p in range(2):
                at = pl.multiple_of((p * twin + group * per + j) * vhead, vhead)
                attn_ref[:, pl.ds(at, vhead)] = jnp.sum(
                    jnp.where(own_line == 2 * row + p, tile, 0.0), axis=0, keepdims=True
                )

    for k in range(rows):
        group = flip(row, k)
        drain(att_all.at[pl.ds(0, 2 if k else 1)], att_rsem.at[k])
        evens, odds = [], []
        for j in range(per):
            tile = jnp.concatenate(
                [att_all[2 * group + c, j].astype(jnp.float32) for c in range(2)], axis=0
            )
            evens.append(jnp.where(both, tile, 0.0).astype(jnp.bfloat16))
            odds.append(jnp.where(both, 0.0, tile).astype(jnp.bfloat16))
        for p, side in enumerate((evens, odds)):
            at = pl.multiple_of((p * twin + group * per) * vhead, per * vhead)
            left = jnp.concatenate(side, axis=1)
            cuts = (0, LANES, columns) if p else (0, columns)
            acc += jnp.concatenate(
                [
                    jnp.dot(
                        left,
                        outw[pl.ds(at, per * vhead), low:high],
                        preferred_element_type=jnp.float32,
                    )
                    for low, high in zip(cuts, cuts[1:])
                ],
                axis=1,
            )
        if k < rows - 1:
            keep(group)
    share = n // heads
    for i in range(heads):
        lots = []
        for token in range(i * share, (i + 1) * share):
            at = token % 2 * lines + token // 2 * 2
            lots.append(acc[at : at + 1] + acc[at + 1 : at + 2])
        part[i] = jnp.concatenate(lots, axis=0)
    swap = remote(part.at[other], part_recv, part_ssem, part_rsem, head=other)
    keep(flip(row, rows - 1))
    swap.wait_recv()
    proj_ref[...] = part[hd] + part_recv[...]
    drain(att_all.at[pl.ds(0, n - 1)], att_ssem)
    swap.wait_send()


def finish(attn_ref, summed_ref, scales_ref, attn_out, proj_out):
    attn_out[...] = attn_ref[...].astype(jnp.bfloat16)
    proj_out[...] = (summed_ref[...] * scales_ref[...].reshape(1, -1)).astype(jnp.bfloat16)


def block(n, heads, *args):
    query, codes, scales, valid, qpos, up, outw, out_scales = args
    own, head_count, width = query.shape
    keys, blocks = scales.shape
    chunk = blocks // 2 + 5
    fits = own == 1 and heads == 2 and n >= 4 and n & (n - 1) == 0 and head_count % n == 0
    fits = fits and width % blocks == 0 and width // blocks % 16 == 0 and blocks > 8
    if not fits:
        return shards(*args)
    vhead = up.shape[2]
    rows, lines = n // 2, n
    per = head_count // n
    columns = outw.shape[1]
    anywhere = pl.BlockSpec(memory_space=pltpu.HBM)
    vmem = pl.BlockSpec(memory_space=pltpu.VMEM)
    dma = pltpu.SemaphoreType.DMA
    attention, summed = pl.pallas_call(
        functools.partial(fused, n, heads),
        out_shape=(
            jax.ShapeDtypeStruct((own, head_count * vhead), jnp.float32),
            jax.ShapeDtypeStruct((n // heads, columns), jnp.float32),
        ),
        in_specs=[anywhere] * 7,
        out_specs=(vmem, vmem),
        scratch_shapes=[
            pltpu.SMEM(valid.shape, jnp.int32),
            pltpu.SMEM(qpos.shape, jnp.int32),
            pltpu.SMEM(valid.shape, jnp.int32),
            pltpu.VMEM((rows, head_count, width), jnp.bfloat16),
            pltpu.VMEM((blocks, width // blocks, keys), jnp.bfloat16),
            pltpu.VMEM((blocks, width // blocks, keys), jnp.bfloat16),
            pltpu.VMEM((blocks, keys), jnp.float32),
            pltpu.VMEM((blocks, keys), jnp.float32),
            pltpu.VMEM(up.shape, jnp.bfloat16),
            pltpu.VMEM(outw.shape, jnp.bfloat16),
            pltpu.VMEM((width, 2 * keys), jnp.bfloat16),
            pltpu.VMEM((LAT_NOPE // LANES, rows * head_count, LANES), jnp.float32),
            pltpu.VMEM((rows * head_count, LANES), jnp.float32),
            pltpu.VMEM((rows * head_count, LANES), jnp.float32),
            pltpu.VMEM((rows, per, lines, vhead), jnp.bfloat16),
            pltpu.VMEM((rows, per, lines, vhead), jnp.bfloat16),
            pltpu.VMEM((rows, lines, LANES), jnp.float32),
            pltpu.VMEM((rows, lines, LANES), jnp.float32),
            pltpu.VMEM((n, per, lines, vhead), jnp.bfloat16),
            pltpu.VMEM((heads, n // heads, columns), jnp.float32),
            pltpu.VMEM((n // heads, columns), jnp.float32),
            pltpu.SemaphoreType.REGULAR((rows + 1,)),
            dma((5,)),
            dma,
            dma,
            dma,
            dma,
            dma((4,)),
            dma((chunk,)),
            dma((2,)),
            dma((chunk - 2,)),
            dma,
            dma,
            dma,
            dma,
            dma,
            dma((rows,)),
            dma,
            dma,
        ],
        compiler_params=pltpu.CompilerParams(
            collective_id=0, has_side_effects=True, vmem_limit_bytes=32 * 1024 * 1024
        ),
        name="mla_block",
    )(
        valid,
        *(
            pltpu.with_memory_space_constraint(operand, pltpu.HBM)
            for operand in (
                qpos,
                query,
                codes.T.reshape(blocks, width // blocks, keys),
                scales.T,
                up,
                outw,
            )
        ),
    )
    return pl.pallas_call(
        finish,
        out_shape=(
            jax.ShapeDtypeStruct((own, head_count * vhead), jnp.bfloat16),
            jax.ShapeDtypeStruct((n // heads, columns), jnp.bfloat16),
        ),
        in_specs=[vmem] * 3,
        out_specs=(vmem, vmem),
        compiler_params=pltpu.CompilerParams(vmem_limit_bytes=1024 * 1024),
        name="finish",
    )(attention, summed, out_scales)


def solution(mesh):
    ctx, heads = mesh.shape["ctx"], mesh.shape["head"]
    return jax.shard_map(
        functools.partial(block, ctx, heads),
        mesh=mesh,
        in_specs=(
            P(("groups", "ctx"), "head", None),
            P(("groups", "ctx"), None),
            P(("groups", "ctx"), None),
            P(("groups", "ctx")),
            P("groups"),
            P("head", None, None),
            P("head", "ctx"),
            P("ctx"),
        ),
        out_specs=(P(("groups", "ctx"), "head"), P(("groups", "head"), "ctx")),
        check_vma=False,
    )
```

```python
import functools
import math

import jax
import jax.numpy as jnp
from jax import lax
from jax.experimental import pallas as pl
from jax.experimental.pallas import tpu as pltpu
from jax.sharding import PartitionSpec as P

LAT_NOPE = 512
ROPE = 64
QK_NOPE = 128
LANES = 128
MASKED = -1e30
FLOOR = -1e29
EXPONENT = math.log2(math.e) * (QK_NOPE + ROPE) ** -0.5
MESH = pl.DeviceIdType.MESH


def shards(
    query_latent,
    latent_codes,
    latent_scales,
    valid_lengths,
    query_position,
    value_up,
    out_codes,
    out_scales,
):
    key_count, width = latent_codes.shape
    block_count = latent_scales.shape[1]
    latent = (
        (
            latent_codes.astype(jnp.float32).reshape(key_count, block_count, width // block_count)
            * latent_scales[:, :, None]
        )
        .reshape(key_count, width)
        .astype(jnp.bfloat16)
    )
    shard_index = lax.axis_index("ctx")
    local_slots = jnp.arange(key_count, dtype=jnp.int32)
    key_pos = shard_index * key_count + local_slots
    usable = local_slots < valid_lengths[0]
    softmax_scale = (QK_NOPE + ROPE) ** (-0.5)
    logits = (
        jnp.einsum(
            "qhc,kc->qhk",
            lax.all_gather(query_latent, "ctx", axis=0, tiled=True),
            latent,
            preferred_element_type=jnp.float32,
        )
        * softmax_scale
    )
    allowed = usable[None, :] & (key_pos[None, :] <= query_position[:, None])
    scores = jnp.where(allowed[:, None, :], logits, -jnp.inf)
    maxima = lax.pmax(jnp.max(scores, axis=2), "ctx")
    weights = jnp.exp(scores - maxima[:, :, None])
    totals = jnp.sum(weights, axis=2)
    latent_mix = jnp.einsum(
        "qhk,kd->qhd",
        weights.astype(jnp.bfloat16),
        latent[:, :LAT_NOPE],
        preferred_element_type=jnp.float32,
    ).astype(jnp.bfloat16)
    values = jnp.einsum("qhd,hdv->qhv", latent_mix, value_up, preferred_element_type=jnp.float32)
    queries, head_count, value_width = values.shape
    numerators = values.reshape(queries, head_count * value_width)
    own_rows = query_latent.shape[0]
    numer_sum, denom_sum = lax.psum((numerators, totals), "ctx")
    attn_all = (
        (numer_sum.reshape(queries, head_count, value_width) / denom_sum[:, :, None])
        .reshape(queries, head_count * value_width)
        .astype(jnp.bfloat16)
    )
    attn_home = lax.dynamic_slice_in_dim(attn_all, shard_index * own_rows, own_rows, 0)
    summed = lax.psum_scatter(
        jnp.dot(attn_all, out_codes, preferred_element_type=jnp.float32),
        "head",
        scatter_dimension=0,
        tiled=True,
    )
    projected = (summed * out_scales[None, :]).astype(jnp.bfloat16)
    return (attn_home, projected)


def flip(index, mask):
    bit, result = 1, index
    while bit <= mask:
        if mask & bit:
            result = result + bit - 2 * bit * lax.rem(index // bit, 2)
        bit *= 2
    return result


def fused(
    n,
    heads,
    valid_hbm,
    qpos_hbm,
    query_hbm,
    codes_hbm,
    scales_hbm,
    up_hbm,
    out_hbm,
    attn_ref,
    proj_ref,
    valid,
    qpos,
    near_valid,
    q_all,
    codes,
    near_codes,
    scales,
    near_scales,
    up,
    outw,
    latent,
    mix,
    stat_m,
    stat_l,
    num_send,
    num_recv,
    st_send,
    st_recv,
    att_all,
    part,
    part_recv,
    sums,
    lent,
    lent_att,
    ready,
    in_sem,
    up_sem,
    out_sem,
    q_ssem,
    q_rsem,
    near_ssem,
    near_rsem,
    half_ssem,
    half_rsem,
    num_ssem,
    num_rsem,
    st_ssem,
    st_rsem,
    att_ssem,
    att_rsem,
    part_ssem,
    part_rsem,
    lent_ssem,
    lent_rsem,
):
    me = lax.axis_index("ctx")
    hd = lax.axis_index("head")
    other = 1 - hd
    row, column = me // 2, lax.rem(me, 2)
    rows = n // 2
    head_count, width = q_all.shape[1:]
    blocks, block, keys = codes.shape
    first = 3 * (blocks - 1) // 8
    units = [(b, min(2, first - b), 0) for b in range(0, first, 2)]
    units += [(b, min(2, blocks - 1 - b), 1) for b in range(first, blocks - 1, 2)]
    rest = pl.ds(blocks - 1, 1)
    nope = mix.shape[0] * LANES
    vhead = up.shape[2]
    twin = head_count // 2
    per = twin // rows
    lines = 2 * rows

    barrier = pltpu.get_barrier_semaphore()
    met = [1] + list(range(2, n, 2))

    def slot_of(k):
        return k if k < 2 else k // 2 + 1

    for k in met:
        later = flip(me, k)

        @pl.when(later > me)
        def _():
            pl.semaphore_signal(barrier, inc=1, device_id={"ctx": later}, device_id_type=MESH)

    @pl.when(hd == 0)
    def _():
        pl.semaphore_signal(barrier, inc=1, device_id={"head": other}, device_id_type=MESH)

    loads = [
        pltpu.make_async_copy(codes_hbm, codes, in_sem.at[0]),
        pltpu.make_async_copy(scales_hbm, scales, in_sem.at[1]),
        pltpu.make_async_copy(query_hbm.at[0], q_all.at[row], in_sem.at[2]),
        pltpu.make_async_copy(valid_hbm, valid, in_sem.at[3]),
        pltpu.make_async_copy(qpos_hbm, qpos, in_sem.at[4]),
    ]
    for copy in loads:
        copy.start()

    ahead = row + column + hd

    @pl.when(ahead > 0)
    def _():
        pl.semaphore_wait(barrier, ahead)

    @pl.when(hd == 1)
    def _():
        pl.semaphore_signal(ready.at[0], inc=1, device_id={"head": other}, device_id_type=MESH)

    for k in met:
        earlier = flip(me, k)

        @pl.when(earlier < me)
        def _():
            pl.semaphore_signal(ready.at[slot_of(k)], inc=1, device_id={"ctx": earlier}, device_id_type=MESH)

    def admit(k):
        @pl.when(flip(me, k) > me)
        def _():
            pl.semaphore_wait(ready.at[slot_of(k)], 1)

    def drain(ref, sem):
        pltpu.make_async_copy(ref, ref, sem).wait()

    def remote(src, dst, ssem, rsem, when=None, **device):
        copy = pltpu.make_async_remote_copy(
            src_ref=src,
            dst_ref=dst,
            send_sem=ssem,
            recv_sem=rsem,
            device_id=device,
            device_id_type=MESH,
        )
        copy.start() if when is None else pl.when(when)(copy.start)
        return copy

    for k in range(rows - 1, 0, -1):
        peer = flip(me, 2 * k)
        remote(query_hbm.at[0], q_all.at[row], q_ssem, q_rsem, peer < me, ctx=peer)

    admit(1)
    partner = flip(me, 1)
    near = [
        remote(valid_hbm, near_valid, near_ssem.at[0], near_rsem.at[0], ctx=partner),
        remote(scales_hbm, near_scales, near_ssem.at[1], near_rsem.at[1], hd == 1, ctx=partner),
    ]
    for p, (b, count, who) in enumerate(units):
        of = pl.ds(b, count)
        near.append(
            remote(
                codes_hbm.at[of],
                near_codes.at[of],
                near_ssem.at[2],
                near_rsem.at[2 + p],
                hd == who,
                ctx=partner,
            )
        )
    last = remote(
        codes_hbm.at[rest],
        near_codes.at[rest],
        near_ssem.at[3],
        near_rsem.at[2 + len(units)],
        ctx=partner,
    )

    up_in = pltpu.make_async_copy(up_hbm, up, up_sem)
    up_in.start()
    loads.pop(2).wait()
    for k in range(1, rows):
        admit(2 * k)
        peer = flip(me, 2 * k)
        remote(q_all.at[row], q_all.at[row], q_ssem, q_rsem, peer > me, ctx=peer)

    out_in = pltpu.make_async_copy(out_hbm, outw, out_sem)
    out_in.start()

    def scale_latent(source, factors, at, of):
        for b in of:
            latent[b * block : (b + 1) * block, at : at + keys] = (
                source[b].astype(jnp.float32) * factors[b : b + 1, :]
            ).astype(jnp.bfloat16)

    for copy in loads:
        copy.wait()
    scale_latent(codes, scales, 0, range(blocks))

    relayed = []

    def relay(ref, index, who):
        pl.when(hd == who)(near[index].wait_recv)
        relayed.append(
            remote(ref, ref, half_ssem.at[min(index, 2) - 1], half_rsem.at[index - 1], hd == who, head=other)
        )

    @pl.when(hd == 0)
    def _():
        pl.semaphore_wait(ready.at[0], 1)

    relay(near_scales, 1, 1)
    for p, (b, count, who) in enumerate(units):
        relay(near_codes.at[pl.ds(b, count)], 2 + p, who)
    pl.when(hd == 0)(relayed[0].wait_recv)
    near[0].wait_recv()
    for p, (b, count, who) in enumerate(units):
        pl.when(hd != who)(relayed[1 + p].wait_recv)
        scale_latent(near_codes, near_scales, keys, range(b, b + count))
    last.wait_recv()
    scale_latent(near_codes, near_scales, keys, range(blocks - 1, blocks))
    drain(q_all.at[pl.ds(0, rows - 1)], q_rsem)
    logits = jnp.dot(
        q_all[...].reshape(rows * head_count, width), latent[...], preferred_element_type=jnp.float32
    )
    slot = lax.broadcasted_iota(jnp.int32, (head_count, 2 * keys), 1)
    weights = []
    for t in range(rows):
        position = qpos[2 * t + column]
        own_limit = jnp.minimum(valid[0], position - me * keys + 1)
        near_limit = jnp.minimum(near_valid[0], position - partner * keys + 1)
        allowed = slot < jnp.where(slot < keys, own_limit, near_limit + keys)
        of = slice(t * head_count, (t + 1) * head_count)
        scores = jnp.where(allowed, logits[of], MASKED)
        top = jnp.maximum(jnp.max(scores, axis=1, keepdims=True), FLOOR)
        weight = jnp.exp2((scores - top) * EXPONENT)
        stat_m[of, :] = jnp.broadcast_to(top, (head_count, LANES))
        stat_l[of, :] = jnp.broadcast_to(jnp.sum(weight, axis=1, keepdims=True), (head_count, LANES))
        weights.append(weight.astype(jnp.bfloat16))
    mixed_all = lax.dot_general(
        jnp.concatenate(weights, axis=0),
        latent[:nope, :],
        (((1,), (1,)), ((), ())),
        preferred_element_type=jnp.float32,
    )
    for c in range(mix.shape[0]):
        mix[c] = mixed_all[:, c * LANES : (c + 1) * LANES]

    up_in.wait()
    tile_lane = lax.broadcasted_iota(jnp.int32, (lines, LANES), 1)
    even = lax.rem(lax.broadcasted_iota(jnp.int32, (lines, LANES), 0), 2) == 0
    for k in range(rows - 1, -1, -1):
        group = flip(row, k)
        stat = jnp.zeros((lines, LANES), jnp.float32)
        for j in range(per):
            of = pl.ds(group * per + j, lines, stride=twin)
            stat = jnp.where(tile_lane == j, stat_m[of, :], stat)
            stat = jnp.where(tile_lane == per + j, stat_l[of, :], stat)
        st_send[k] = stat
        if k:
            remote(st_send.at[k], st_recv.at[k], st_ssem, st_rsem, ctx=flip(me, 2 * k))
        for j in range(per):
            h = group * per + j
            of = pl.ds(h, lines, stride=twin)
            mixed = jnp.concatenate(
                [mix[c, of, :] for c in range(mix.shape[0])], axis=1
            ).astype(jnp.bfloat16)
            pair = jnp.dot(
                mixed,
                jnp.concatenate([up[h], up[h + twin]], axis=1),
                preferred_element_type=jnp.float32,
            )
            num_send[k, j] = jnp.where(even, pair[:, :vhead], pair[:, vhead:]).astype(jnp.bfloat16)
        if k:
            remote(num_send.at[k], num_recv.at[k], num_ssem, num_rsem, ctx=flip(me, 2 * k))

    @pl.when(hd == 0)
    def _():
        for p in range(2):
            at = (p * twin + flip(row, 1) * per) * vhead
            remote(
                out_hbm.at[pl.ds(pl.multiple_of(at, per * vhead), per * vhead)],
                lent.at[p],
                lent_ssem.at[0],
                lent_rsem.at[0],
                head=other,
            )

    drain(st_recv.at[pl.ds(1, rows - 1)], st_rsem)
    drain(num_recv.at[pl.ds(1, rows - 1)], num_rsem)

    stats = [st_send[0]] + [st_recv[k] for k in range(1, rows)]
    top = functools.reduce(jnp.maximum, stats)
    factors = [jnp.exp2((s - top) * EXPONENT) for s in stats]
    for j in range(per):
        total = jnp.zeros((lines, 1), jnp.float32)
        value = jnp.zeros((lines, vhead), jnp.float32)
        for k, (s, f) in enumerate(zip(stats, factors)):
            factor = f[:, j : j + 1]
            total += factor * s[:, per + j : per + j + 1]
            value += factor * (num_recv if k else num_send)[k, j].astype(jnp.float32)
        att_all[me, j] = (value / total).astype(jnp.bfloat16)

    for k in range(n - 1, 0, -1):
        remote(
            att_all.at[me],
            att_all.at[me],
            att_ssem,
            att_rsem.at[k // 2],
            None if k != 3 else hd == 1,
            ctx=flip(me, k),
        )

    @pl.when(hd == 0)
    def _():
        for target in (flip(me, 3), flip(me, 2)):
            remote(
                att_all.at[me],
                lent_att.at[column],
                lent_ssem.at[1],
                lent_rsem.at[1],
                ctx=target,
                head=other,
            )

    for copy in [near[0], last]:
        copy.wait_send()
    drain(q_all.at[pl.ds(0, rows - 1)], q_ssem)
    drain(st_send.at[pl.ds(1, rows - 1)], st_ssem)
    drain(num_send.at[pl.ds(1, rows - 1)], num_ssem)

    @pl.when(hd == 0)
    def _():
        ours = near_codes.at[pl.ds(0, first)]
        drain(ours, near_ssem.at[2])
        drain(ours, half_ssem.at[1])

    @pl.when(hd == 1)
    def _():
        ours = near_codes.at[pl.ds(first, blocks - 1 - first)]
        drain(near_scales, near_ssem.at[1])
        drain(near_scales, half_ssem.at[0])
        drain(ours, near_ssem.at[2])
        drain(ours, half_ssem.at[1])

    out_in.wait()
    columns = outw.shape[1]
    acc = jnp.zeros((2 * lines, columns), jnp.float32)
    both = lax.rem(lax.broadcasted_iota(jnp.int32, (2 * lines, LANES), 0), 2) == 0
    own_line = lax.broadcasted_iota(jnp.int32, (lines, LANES), 0)

    def keep(group):
        for j in range(per):
            tile = att_all[2 * group + column, j].astype(jnp.float32)
            for p in range(2):
                at = pl.multiple_of((p * twin + group * per + j) * vhead, vhead)
                attn_ref[:, pl.ds(at, vhead)] = jnp.sum(
                    jnp.where(own_line == 2 * row + p, tile, 0.0), axis=0, keepdims=True
                )

    def product(piece, weight):
        evens, odds = [], []
        for j in range(per):
            tile = jnp.concatenate([piece(c, j).astype(jnp.float32) for c in range(2)], axis=0)
            evens.append(jnp.where(both, tile, 0.0).astype(jnp.bfloat16))
            odds.append(jnp.where(both, 0.0, tile).astype(jnp.bfloat16))
        out = jnp.zeros((2 * lines, columns), jnp.float32)
        for p, side in enumerate((evens, odds)):
            left = jnp.concatenate(side, axis=1)
            cuts = (0, LANES, columns) if p else (0, columns)
            out += jnp.concatenate(
                [
                    jnp.dot(left, weight(p, low, high), preferred_element_type=jnp.float32)
                    for low, high in zip(cuts, cuts[1:])
                ],
                axis=1,
            )
        return out

    def arrive(k, count=2):
        drain(att_all.at[pl.ds(0, count if k else 1)], att_rsem.at[k])

    def project(k):
        group = flip(row, k)
        arrive(k)

        def weight(p, low, high):
            at = pl.multiple_of((p * twin + group * per) * vhead, per * vhead)
            return outw[pl.ds(at, per * vhead), low:high]

        return product(lambda c, j: att_all[2 * group + c, j], weight)

    sums[...] = acc + project(0)
    keep(row)

    @pl.when(hd == 1)
    def _():
        sums[...] += project(1)

    acc = sums[...]
    for k in range(2, rows):
        acc += project(k)
        if k < rows - 1:
            keep(flip(row, k))
    sums[...] = acc

    @pl.when(hd == 1)
    def _():
        drain(lent, lent_rsem.at[0])
        drain(lent_att, lent_rsem.at[1])
        sums[...] += product(lambda c, j: lent_att[c, j], lambda p, low, high: lent[p, :, low:high])

    acc = sums[...]
    share = n // heads
    for i in range(heads):
        lots = []
        for token in range(i * share, (i + 1) * share):
            at = token % 2 * lines + token // 2 * 2
            lots.append(acc[at : at + 1] + acc[at + 1 : at + 2])
        part[i] = jnp.concatenate(lots, axis=0)
    swap = remote(part.at[other], part_recv, part_ssem, part_rsem, head=other)
    pl.when(hd == 0)(lambda: arrive(1, 1))
    for k in (1, rows - 1):
        keep(flip(row, k))
    swap.wait_recv()
    proj_ref[...] = part[hd] + part_recv[...]
    drain(att_all.at[pl.ds(0, n - 2)], att_ssem)

    @pl.when(hd == 0)
    def _():
        drain(lent, lent_ssem.at[0])
        drain(lent_att, lent_ssem.at[1])

    pl.when(hd == 1)(lambda: drain(att_all.at[pl.ds(0, 1)], att_ssem))
    swap.wait_send()


def finish(attn_ref, summed_ref, scales_ref, attn_out, proj_out):
    attn_out[...] = attn_ref[...].astype(jnp.bfloat16)
    proj_out[...] = (summed_ref[...] * scales_ref[...].reshape(1, -1)).astype(jnp.bfloat16)


def block(n, heads, *args):
    query, codes, scales, valid, qpos, up, outw, out_scales = args
    own, head_count, width = query.shape
    keys, blocks = scales.shape
    chunk = blocks // 2 + 5
    fits = own == 1 and heads == 2 and n >= 4 and n & (n - 1) == 0 and head_count % n == 0
    fits = fits and width % blocks == 0 and width // blocks % 16 == 0 and blocks > 8
    if not fits:
        return shards(*args)
    vhead = up.shape[2]
    rows, lines = n // 2, n
    per = head_count // n
    columns = outw.shape[1]
    anywhere = pl.BlockSpec(memory_space=pltpu.HBM)
    vmem = pl.BlockSpec(memory_space=pltpu.VMEM)
    dma = pltpu.SemaphoreType.DMA
    attention, summed = pl.pallas_call(
        functools.partial(fused, n, heads),
        out_shape=(
            jax.ShapeDtypeStruct((own, head_count * vhead), jnp.float32),
            jax.ShapeDtypeStruct((n // heads, columns), jnp.float32),
        ),
        in_specs=[anywhere] * 7,
        out_specs=(vmem, vmem),
        scratch_shapes=[
            pltpu.SMEM(valid.shape, jnp.int32),
            pltpu.SMEM(qpos.shape, jnp.int32),
            pltpu.SMEM(valid.shape, jnp.int32),
            pltpu.VMEM((rows, head_count, width), jnp.bfloat16),
            pltpu.VMEM((blocks, width // blocks, keys), jnp.bfloat16),
            pltpu.VMEM((blocks, width // blocks, keys), jnp.bfloat16),
            pltpu.VMEM((blocks, keys), jnp.float32),
            pltpu.VMEM((blocks, keys), jnp.float32),
            pltpu.VMEM(up.shape, jnp.bfloat16),
            pltpu.VMEM(outw.shape, jnp.bfloat16),
            pltpu.VMEM((width, 2 * keys), jnp.bfloat16),
            pltpu.VMEM((LAT_NOPE // LANES, rows * head_count, LANES), jnp.float32),
            pltpu.VMEM((rows * head_count, LANES), jnp.float32),
            pltpu.VMEM((rows * head_count, LANES), jnp.float32),
            pltpu.VMEM((rows, per, lines, vhead), jnp.bfloat16),
            pltpu.VMEM((rows, per, lines, vhead), jnp.bfloat16),
            pltpu.VMEM((rows, lines, LANES), jnp.float32),
            pltpu.VMEM((rows, lines, LANES), jnp.float32),
            pltpu.VMEM((n, per, lines, vhead), jnp.bfloat16),
            pltpu.VMEM((heads, n // heads, columns), jnp.float32),
            pltpu.VMEM((n // heads, columns), jnp.float32),
            pltpu.VMEM((n * 2, columns), jnp.float32),
            pltpu.VMEM((2, per * vhead, columns), jnp.bfloat16),
            pltpu.VMEM((2, per, lines, vhead), jnp.bfloat16),
            pltpu.SemaphoreType.REGULAR((rows + 1,)),
            dma((5,)),
            dma,
            dma,
            dma,
            dma,
            dma((4,)),
            dma((chunk,)),
            dma((2,)),
            dma((chunk - 2,)),
            dma,
            dma,
            dma,
            dma,
            dma,
            dma((rows,)),
            dma,
            dma,
            dma((2,)),
            dma((2,)),
        ],
        compiler_params=pltpu.CompilerParams(
            collective_id=0, has_side_effects=True, vmem_limit_bytes=32 * 1024 * 1024
        ),
        name="mla_block",
    )(
        valid,
        *(
            pltpu.with_memory_space_constraint(operand, pltpu.HBM)
            for operand in (
                qpos,
                query,
                codes.T.reshape(blocks, width // blocks, keys),
                scales.T,
                up,
                outw,
            )
        ),
    )
    return pl.pallas_call(
        finish,
        out_shape=(
            jax.ShapeDtypeStruct((own, head_count * vhead), jnp.bfloat16),
            jax.ShapeDtypeStruct((n // heads, columns), jnp.bfloat16),
        ),
        in_specs=[vmem] * 3,
        out_specs=(vmem, vmem),
        compiler_params=pltpu.CompilerParams(vmem_limit_bytes=1024 * 1024),
        name="finish",
    )(attention, summed, out_scales)


def solution(mesh):
    ctx, heads = mesh.shape["ctx"], mesh.shape["head"]
    return jax.shard_map(
        functools.partial(block, ctx, heads),
        mesh=mesh,
        in_specs=(
            P(("groups", "ctx"), "head", None),
            P(("groups", "ctx"), None),
            P(("groups", "ctx"), None),
            P(("groups", "ctx")),
            P("groups"),
            P("head", None, None),
            P("head", "ctx"),
            P("ctx"),
        ),
        out_specs=(P(("groups", "ctx"), "head"), P(("groups", "head"), "ctx")),
        check_vma=False,
    )
```

```python
import functools
import math

import jax
import jax.numpy as jnp
from jax import lax
from jax.experimental import pallas as pl
from jax.experimental.pallas import tpu as pltpu
from jax.sharding import PartitionSpec as P

LAT_NOPE = 512
ROPE = 64
QK_NOPE = 128
LANES = 128
MASKED = -1e30
FLOOR = -1e29
EXPONENT = math.log2(math.e) * (QK_NOPE + ROPE) ** -0.5
MESH = pl.DeviceIdType.MESH


def shards(
    query_latent,
    latent_codes,
    latent_scales,
    valid_lengths,
    query_position,
    value_up,
    out_codes,
    out_scales,
):
    key_count, width = latent_codes.shape
    block_count = latent_scales.shape[1]
    latent = (
        (
            latent_codes.astype(jnp.float32).reshape(key_count, block_count, width // block_count)
            * latent_scales[:, :, None]
        )
        .reshape(key_count, width)
        .astype(jnp.bfloat16)
    )
    shard_index = lax.axis_index("ctx")
    local_slots = jnp.arange(key_count, dtype=jnp.int32)
    key_pos = shard_index * key_count + local_slots
    usable = local_slots < valid_lengths[0]
    softmax_scale = (QK_NOPE + ROPE) ** (-0.5)
    logits = (
        jnp.einsum(
            "qhc,kc->qhk",
            lax.all_gather(query_latent, "ctx", axis=0, tiled=True),
            latent,
            preferred_element_type=jnp.float32,
        )
        * softmax_scale
    )
    allowed = usable[None, :] & (key_pos[None, :] <= query_position[:, None])
    scores = jnp.where(allowed[:, None, :], logits, -jnp.inf)
    maxima = lax.pmax(jnp.max(scores, axis=2), "ctx")
    weights = jnp.exp(scores - maxima[:, :, None])
    totals = jnp.sum(weights, axis=2)
    latent_mix = jnp.einsum(
        "qhk,kd->qhd",
        weights.astype(jnp.bfloat16),
        latent[:, :LAT_NOPE],
        preferred_element_type=jnp.float32,
    ).astype(jnp.bfloat16)
    values = jnp.einsum("qhd,hdv->qhv", latent_mix, value_up, preferred_element_type=jnp.float32)
    queries, head_count, value_width = values.shape
    numerators = values.reshape(queries, head_count * value_width)
    own_rows = query_latent.shape[0]
    numer_sum, denom_sum = lax.psum((numerators, totals), "ctx")
    attn_all = (
        (numer_sum.reshape(queries, head_count, value_width) / denom_sum[:, :, None])
        .reshape(queries, head_count * value_width)
        .astype(jnp.bfloat16)
    )
    attn_home = lax.dynamic_slice_in_dim(attn_all, shard_index * own_rows, own_rows, 0)
    summed = lax.psum_scatter(
        jnp.dot(attn_all, out_codes, preferred_element_type=jnp.float32),
        "head",
        scatter_dimension=0,
        tiled=True,
    )
    projected = (summed * out_scales[None, :]).astype(jnp.bfloat16)
    return (attn_home, projected)


def flip(index, mask):
    bit, result = 1, index
    while bit <= mask:
        if mask & bit:
            result = result + bit - 2 * bit * lax.rem(index // bit, 2)
        bit *= 2
    return result


def fused(
    n,
    heads,
    valid_hbm,
    qpos_hbm,
    query_hbm,
    codes_hbm,
    scales_hbm,
    up_hbm,
    out_hbm,
    attn_ref,
    proj_ref,
    valid,
    qpos,
    near_valid,
    q_all,
    codes,
    near_codes,
    scales,
    near_scales,
    up,
    outw,
    latent,
    mix,
    stat_m,
    stat_l,
    num_send,
    num_recv,
    st_send,
    st_recv,
    att_all,
    part,
    part_recv,
    sums,
    lent,
    lent_att,
    ready,
    in_sem,
    up_sem,
    out_sem,
    q_ssem,
    q_rsem,
    near_ssem,
    near_rsem,
    half_ssem,
    half_rsem,
    num_ssem,
    num_rsem,
    st_ssem,
    st_rsem,
    att_ssem,
    att_rsem,
    part_ssem,
    part_rsem,
    lent_ssem,
    lent_rsem,
):
    me = lax.axis_index("ctx")
    hd = lax.axis_index("head")
    other = 1 - hd
    row, column = me // 2, lax.rem(me, 2)
    rows = n // 2
    head_count, width = q_all.shape[1:]
    blocks, block, keys = codes.shape
    first = 3 * (blocks - 1) // 8
    units = [(b, min(2, first - b), 0) for b in range(0, first, 2)]
    units += [(b, min(2, blocks - 1 - b), 1) for b in range(first, blocks - 1, 2)]
    rest = pl.ds(blocks - 1, 1)
    nope = mix.shape[0] * LANES
    vhead = up.shape[2]
    twin = head_count // 2
    per = twin // rows
    lines = 2 * rows

    barrier = pltpu.get_barrier_semaphore()
    met = [1] + list(range(2, n, 2))

    def slot_of(k):
        return k if k < 2 else k // 2 + 1

    for k in met:
        later = flip(me, k)

        @pl.when(later > me)
        def _():
            pl.semaphore_signal(barrier, inc=1, device_id={"ctx": later}, device_id_type=MESH)

    @pl.when(hd == 0)
    def _():
        pl.semaphore_signal(barrier, inc=1, device_id={"head": other}, device_id_type=MESH)

    loads = [
        pltpu.make_async_copy(codes_hbm, codes, in_sem.at[0]),
        pltpu.make_async_copy(scales_hbm, scales, in_sem.at[1]),
        pltpu.make_async_copy(query_hbm.at[0], q_all.at[row], in_sem.at[2]),
        pltpu.make_async_copy(valid_hbm, valid, in_sem.at[3]),
        pltpu.make_async_copy(qpos_hbm, qpos, in_sem.at[4]),
    ]
    for copy in loads:
        copy.start()

    ahead = row + column + hd

    @pl.when(ahead > 0)
    def _():
        pl.semaphore_wait(barrier, ahead)

    @pl.when(hd == 1)
    def _():
        pl.semaphore_signal(ready.at[0], inc=1, device_id={"head": other}, device_id_type=MESH)

    for k in met:
        earlier = flip(me, k)

        @pl.when(earlier < me)
        def _():
            pl.semaphore_signal(ready.at[slot_of(k)], inc=1, device_id={"ctx": earlier}, device_id_type=MESH)

    def admit(k):
        @pl.when(flip(me, k) > me)
        def _():
            pl.semaphore_wait(ready.at[slot_of(k)], 1)

    def drain(ref, sem):
        pltpu.make_async_copy(ref, ref, sem).wait()

    def remote(src, dst, ssem, rsem, when=None, **device):
        copy = pltpu.make_async_remote_copy(
            src_ref=src,
            dst_ref=dst,
            send_sem=ssem,
            recv_sem=rsem,
            device_id=device,
            device_id_type=MESH,
        )
        copy.start() if when is None else pl.when(when)(copy.start)
        return copy

    for k in range(rows - 1, 0, -1):
        peer = flip(me, 2 * k)
        remote(query_hbm.at[0], q_all.at[row], q_ssem, q_rsem, peer < me, ctx=peer)

    admit(1)
    partner = flip(me, 1)
    near = [
        remote(valid_hbm, near_valid, near_ssem.at[0], near_rsem.at[0], ctx=partner),
        remote(scales_hbm, near_scales, near_ssem.at[1], near_rsem.at[1], hd == 1, ctx=partner),
    ]
    for p, (b, count, who) in enumerate(units):
        of = pl.ds(b, count)
        near.append(
            remote(
                codes_hbm.at[of],
                near_codes.at[of],
                near_ssem.at[2],
                near_rsem.at[2 + p],
                hd == who,
                ctx=partner,
            )
        )
    last = remote(
        codes_hbm.at[rest],
        near_codes.at[rest],
        near_ssem.at[3],
        near_rsem.at[2 + len(units)],
        ctx=partner,
    )

    up_in = pltpu.make_async_copy(up_hbm, up, up_sem)
    up_in.start()
    loads.pop(2).wait()
    for k in range(1, rows):
        admit(2 * k)
        peer = flip(me, 2 * k)
        remote(q_all.at[row], q_all.at[row], q_ssem, q_rsem, peer > me, ctx=peer)

    out_in = pltpu.make_async_copy(out_hbm, outw, out_sem)
    out_in.start()

    def scale_latent(source, factors, at, of):
        for b in of:
            latent[b * block : (b + 1) * block, at : at + keys] = (
                source[b].astype(jnp.float32) * factors[b : b + 1, :]
            ).astype(jnp.bfloat16)

    for copy in loads:
        copy.wait()
    scale_latent(codes, scales, 0, range(blocks))

    relayed = []

    def relay(ref, index, who):
        pl.when(hd == who)(near[index].wait_recv)
        relayed.append(
            remote(ref, ref, half_ssem.at[min(index, 2) - 1], half_rsem.at[index - 1], hd == who, head=other)
        )

    @pl.when(hd == 0)
    def _():
        pl.semaphore_wait(ready.at[0], 1)

    relay(near_scales, 1, 1)
    for p, (b, count, who) in enumerate(units):
        relay(near_codes.at[pl.ds(b, count)], 2 + p, who)
    pl.when(hd == 0)(relayed[0].wait_recv)
    near[0].wait_recv()
    for p, (b, count, who) in enumerate(units):
        pl.when(hd != who)(relayed[1 + p].wait_recv)
        scale_latent(near_codes, near_scales, keys, range(b, b + count))
    last.wait_recv()
    scale_latent(near_codes, near_scales, keys, range(blocks - 1, blocks))
    drain(q_all.at[pl.ds(0, rows - 1)], q_rsem)
    logits = jnp.dot(
        q_all[...].reshape(rows * head_count, width), latent[...], preferred_element_type=jnp.float32
    )
    slot = lax.broadcasted_iota(jnp.int32, (head_count, 2 * keys), 1)
    weights = []
    for t in range(rows):
        position = qpos[2 * t + column]
        own_limit = jnp.minimum(valid[0], position - me * keys + 1)
        near_limit = jnp.minimum(near_valid[0], position - partner * keys + 1)
        allowed = slot < jnp.where(slot < keys, own_limit, near_limit + keys)
        of = slice(t * head_count, (t + 1) * head_count)
        scores = jnp.where(allowed, logits[of], MASKED)
        top = jnp.maximum(jnp.max(scores, axis=1, keepdims=True), FLOOR)
        weight = jnp.exp2((scores - top) * EXPONENT)
        stat_m[of, :] = jnp.broadcast_to(top, (head_count, LANES))
        stat_l[of, :] = jnp.broadcast_to(jnp.sum(weight, axis=1, keepdims=True), (head_count, LANES))
        weights.append(weight.astype(jnp.bfloat16))
    mixed_all = lax.dot_general(
        jnp.concatenate(weights, axis=0),
        latent[:nope, :],
        (((1,), (1,)), ((), ())),
        preferred_element_type=jnp.float32,
    )
    for c in range(mix.shape[0]):
        mix[c] = mixed_all[:, c * LANES : (c + 1) * LANES]

    up_in.wait()
    tile_lane = lax.broadcasted_iota(jnp.int32, (lines, LANES), 1)
    even = lax.rem(lax.broadcasted_iota(jnp.int32, (lines, LANES), 0), 2) == 0
    for k in range(rows - 1, -1, -1):
        group = flip(row, k)
        stat = jnp.zeros((lines, LANES), jnp.float32)
        for j in range(per):
            of = pl.ds(group * per + j, lines, stride=twin)
            stat = jnp.where(tile_lane == j, stat_m[of, :], stat)
            stat = jnp.where(tile_lane == per + j, stat_l[of, :], stat)
        st_send[k] = stat
        if k:
            remote(st_send.at[k], st_recv.at[k], st_ssem, st_rsem, ctx=flip(me, 2 * k))
        for j in range(per):
            h = group * per + j
            of = pl.ds(h, lines, stride=twin)
            mixed = jnp.concatenate(
                [mix[c, of, :] for c in range(mix.shape[0])], axis=1
            ).astype(jnp.bfloat16)
            pair = jnp.dot(
                mixed,
                jnp.concatenate([up[h], up[h + twin]], axis=1),
                preferred_element_type=jnp.float32,
            )
            num_send[k, j] = jnp.where(even, pair[:, :vhead], pair[:, vhead:]).astype(jnp.bfloat16)
        if k:
            remote(num_send.at[k], num_recv.at[k], num_ssem, num_rsem, ctx=flip(me, 2 * k))

    @pl.when(hd == 0)
    def _():
        for p in range(2):
            at = (p * twin + flip(row, rows - 1) * per) * vhead
            remote(
                out_hbm.at[pl.ds(pl.multiple_of(at, per * vhead), per * vhead)],
                lent.at[p],
                lent_ssem.at[0],
                lent_rsem.at[0],
                head=other,
            )

    drain(st_recv.at[pl.ds(1, rows - 1)], st_rsem)
    drain(num_recv.at[pl.ds(1, rows - 1)], num_rsem)

    stats = [st_send[0]] + [st_recv[k] for k in range(1, rows)]
    top = functools.reduce(jnp.maximum, stats)
    factors = [jnp.exp2((s - top) * EXPONENT) for s in stats]
    for j in range(per):
        total = jnp.zeros((lines, 1), jnp.float32)
        value = jnp.zeros((lines, vhead), jnp.float32)
        for k, (s, f) in enumerate(zip(stats, factors)):
            factor = f[:, j : j + 1]
            total += factor * s[:, per + j : per + j + 1]
            value += factor * (num_recv if k else num_send)[k, j].astype(jnp.float32)
        att_all[me, j] = (value / total).astype(jnp.bfloat16)

    @pl.when(hd == 0)
    def _():
        for target in (flip(me, n - 1), flip(me, n - 2)):
            remote(
                att_all.at[me],
                lent_att.at[column],
                lent_ssem.at[1],
                lent_rsem.at[1],
                ctx=target,
                head=other,
            )

    for k in range(n - 1, 0, -1):
        remote(
            att_all.at[me],
            att_all.at[me],
            att_ssem,
            att_rsem.at[k // 2],
            None if k < n - 1 else hd == 1,
            ctx=flip(me, k),
        )

    for copy in [near[0], last]:
        copy.wait_send()
    drain(q_all.at[pl.ds(0, rows - 1)], q_ssem)
    drain(st_send.at[pl.ds(1, rows - 1)], st_ssem)
    drain(num_send.at[pl.ds(1, rows - 1)], num_ssem)

    @pl.when(hd == 0)
    def _():
        ours = near_codes.at[pl.ds(0, first)]
        drain(ours, near_ssem.at[2])
        drain(ours, half_ssem.at[1])

    @pl.when(hd == 1)
    def _():
        ours = near_codes.at[pl.ds(first, blocks - 1 - first)]
        drain(near_scales, near_ssem.at[1])
        drain(near_scales, half_ssem.at[0])
        drain(ours, near_ssem.at[2])
        drain(ours, half_ssem.at[1])

    out_in.wait()
    columns = outw.shape[1]
    acc = jnp.zeros((2 * lines, columns), jnp.float32)
    both = lax.rem(lax.broadcasted_iota(jnp.int32, (2 * lines, LANES), 0), 2) == 0
    own_line = lax.broadcasted_iota(jnp.int32, (lines, LANES), 0)

    def keep(group):
        for j in range(per):
            tile = att_all[2 * group + column, j].astype(jnp.float32)
            for p in range(2):
                at = pl.multiple_of((p * twin + group * per + j) * vhead, vhead)
                attn_ref[:, pl.ds(at, vhead)] = jnp.sum(
                    jnp.where(own_line == 2 * row + p, tile, 0.0), axis=0, keepdims=True
                )

    def product(piece, weight):
        evens, odds = [], []
        for j in range(per):
            tile = jnp.concatenate([piece(c, j).astype(jnp.float32) for c in range(2)], axis=0)
            evens.append(jnp.where(both, tile, 0.0).astype(jnp.bfloat16))
            odds.append(jnp.where(both, 0.0, tile).astype(jnp.bfloat16))
        out = jnp.zeros((2 * lines, columns), jnp.float32)
        for p, side in enumerate((evens, odds)):
            left = jnp.concatenate(side, axis=1)
            cuts = (0, LANES, columns) if p else (0, columns)
            out += jnp.concatenate(
                [
                    jnp.dot(left, weight(p, low, high), preferred_element_type=jnp.float32)
                    for low, high in zip(cuts, cuts[1:])
                ],
                axis=1,
            )
        return out

    def arrive(k, count=2):
        drain(att_all.at[pl.ds(0, count if k else 1)], att_rsem.at[k])

    def project(k):
        group = flip(row, k)
        arrive(k)

        def weight(p, low, high):
            at = pl.multiple_of((p * twin + group * per) * vhead, per * vhead)
            return outw[pl.ds(at, per * vhead), low:high]

        return product(lambda c, j: att_all[2 * group + c, j], weight)

    for k in range(rows - 1):
        acc += project(k)
        if k < rows - 2:
            keep(flip(row, k))
    sums[...] = acc

    @pl.when(hd == 1)
    def _():
        sums[...] += project(rows - 1)
        drain(lent, lent_rsem.at[0])
        drain(lent_att, lent_rsem.at[1])
        sums[...] += product(lambda c, j: lent_att[c, j], lambda p, low, high: lent[p, :, low:high])

    acc = sums[...]
    share = n // heads
    for i in range(heads):
        lots = []
        for token in range(i * share, (i + 1) * share):
            at = token % 2 * lines + token // 2 * 2
            lots.append(acc[at : at + 1] + acc[at + 1 : at + 2])
        part[i] = jnp.concatenate(lots, axis=0)
    swap = remote(part.at[other], part_recv, part_ssem, part_rsem, head=other)
    pl.when(hd == 0)(lambda: arrive(rows - 1, 1))
    for k in (rows - 2, rows - 1):
        keep(flip(row, k))
    swap.wait_recv()
    proj_ref[...] = part[hd] + part_recv[...]
    drain(att_all.at[pl.ds(0, n - 2)], att_ssem)

    @pl.when(hd == 0)
    def _():
        drain(lent, lent_ssem.at[0])
        drain(lent_att, lent_ssem.at[1])

    pl.when(hd == 1)(lambda: drain(att_all.at[pl.ds(0, 1)], att_ssem))
    swap.wait_send()


def finish(attn_ref, summed_ref, scales_ref, attn_out, proj_out):
    attn_out[...] = attn_ref[...].astype(jnp.bfloat16)
    proj_out[...] = (summed_ref[...] * scales_ref[...].reshape(1, -1)).astype(jnp.bfloat16)


def block(n, heads, *args):
    query, codes, scales, valid, qpos, up, outw, out_scales = args
    own, head_count, width = query.shape
    keys, blocks = scales.shape
    chunk = blocks // 2 + 5
    fits = own == 1 and heads == 2 and n >= 4 and n & (n - 1) == 0 and head_count % n == 0
    fits = fits and width % blocks == 0 and width // blocks % 16 == 0 and blocks > 8
    if not fits:
        return shards(*args)
    vhead = up.shape[2]
    rows, lines = n // 2, n
    per = head_count // n
    columns = outw.shape[1]
    anywhere = pl.BlockSpec(memory_space=pltpu.HBM)
    vmem = pl.BlockSpec(memory_space=pltpu.VMEM)
    dma = pltpu.SemaphoreType.DMA
    attention, summed = pl.pallas_call(
        functools.partial(fused, n, heads),
        out_shape=(
            jax.ShapeDtypeStruct((own, head_count * vhead), jnp.float32),
            jax.ShapeDtypeStruct((n // heads, columns), jnp.float32),
        ),
        in_specs=[anywhere] * 7,
        out_specs=(vmem, vmem),
        scratch_shapes=[
            pltpu.SMEM(valid.shape, jnp.int32),
            pltpu.SMEM(qpos.shape, jnp.int32),
            pltpu.SMEM(valid.shape, jnp.int32),
            pltpu.VMEM((rows, head_count, width), jnp.bfloat16),
            pltpu.VMEM((blocks, width // blocks, keys), jnp.bfloat16),
            pltpu.VMEM((blocks, width // blocks, keys), jnp.bfloat16),
            pltpu.VMEM((blocks, keys), jnp.float32),
            pltpu.VMEM((blocks, keys), jnp.float32),
            pltpu.VMEM(up.shape, jnp.bfloat16),
            pltpu.VMEM(outw.shape, jnp.bfloat16),
            pltpu.VMEM((width, 2 * keys), jnp.bfloat16),
            pltpu.VMEM((LAT_NOPE // LANES, rows * head_count, LANES), jnp.float32),
            pltpu.VMEM((rows * head_count, LANES), jnp.float32),
            pltpu.VMEM((rows * head_count, LANES), jnp.float32),
            pltpu.VMEM((rows, per, lines, vhead), jnp.bfloat16),
            pltpu.VMEM((rows, per, lines, vhead), jnp.bfloat16),
            pltpu.VMEM((rows, lines, LANES), jnp.float32),
            pltpu.VMEM((rows, lines, LANES), jnp.float32),
            pltpu.VMEM((n, per, lines, vhead), jnp.bfloat16),
            pltpu.VMEM((heads, n // heads, columns), jnp.float32),
            pltpu.VMEM((n // heads, columns), jnp.float32),
            pltpu.VMEM((n * 2, columns), jnp.float32),
            pltpu.VMEM((2, per * vhead, columns), jnp.bfloat16),
            pltpu.VMEM((2, per, lines, vhead), jnp.bfloat16),
            pltpu.SemaphoreType.REGULAR((rows + 1,)),
            dma((5,)),
            dma,
            dma,
            dma,
            dma,
            dma((4,)),
            dma((chunk,)),
            dma((2,)),
            dma((chunk - 2,)),
            dma,
            dma,
            dma,
            dma,
            dma,
            dma((rows,)),
            dma,
            dma,
            dma((2,)),
            dma((2,)),
        ],
        compiler_params=pltpu.CompilerParams(
            collective_id=0, has_side_effects=True, vmem_limit_bytes=32 * 1024 * 1024
        ),
        name="mla_block",
    )(
        valid,
        *(
            pltpu.with_memory_space_constraint(operand, pltpu.HBM)
            for operand in (
                qpos,
                query,
                codes.T.reshape(blocks, width // blocks, keys),
                scales.T,
                up,
                outw,
            )
        ),
    )
    return pl.pallas_call(
        finish,
        out_shape=(
            jax.ShapeDtypeStruct((own, head_count * vhead), jnp.bfloat16),
            jax.ShapeDtypeStruct((n // heads, columns), jnp.bfloat16),
        ),
        in_specs=[vmem] * 3,
        out_specs=(vmem, vmem),
        compiler_params=pltpu.CompilerParams(vmem_limit_bytes=1024 * 1024),
        name="finish",
    )(attention, summed, out_scales)


def solution(mesh):
    ctx, heads = mesh.shape["ctx"], mesh.shape["head"]
    return jax.shard_map(
        functools.partial(block, ctx, heads),
        mesh=mesh,
        in_specs=(
            P(("groups", "ctx"), "head", None),
            P(("groups", "ctx"), None),
            P(("groups", "ctx"), None),
            P(("groups", "ctx")),
            P("groups"),
            P("head", None, None),
            P("head", "ctx"),
            P("ctx"),
        ),
        out_specs=(P(("groups", "ctx"), "head"), P(("groups", "head"), "ctx")),
        check_vma=False,
    )
```

```python
import functools
import math

import jax
import jax.numpy as jnp
from jax import lax
from jax.experimental import pallas as pl
from jax.experimental.pallas import tpu as pltpu
from jax.sharding import PartitionSpec as P

LAT_NOPE = 512
ROPE = 64
QK_NOPE = 128
LANES = 128
MASKED = -1e30
FLOOR = -1e29
EXPONENT = math.log2(math.e) * (QK_NOPE + ROPE) ** -0.5
MESH = pl.DeviceIdType.MESH


def shards(
    query_latent,
    latent_codes,
    latent_scales,
    valid_lengths,
    query_position,
    value_up,
    out_codes,
    out_scales,
):
    key_count, width = latent_codes.shape
    block_count = latent_scales.shape[1]
    latent = (
        (
            latent_codes.astype(jnp.float32).reshape(key_count, block_count, width // block_count)
            * latent_scales[:, :, None]
        )
        .reshape(key_count, width)
        .astype(jnp.bfloat16)
    )
    shard_index = lax.axis_index("ctx")
    local_slots = jnp.arange(key_count, dtype=jnp.int32)
    key_pos = shard_index * key_count + local_slots
    usable = local_slots < valid_lengths[0]
    softmax_scale = (QK_NOPE + ROPE) ** (-0.5)
    logits = (
        jnp.einsum(
            "qhc,kc->qhk",
            lax.all_gather(query_latent, "ctx", axis=0, tiled=True),
            latent,
            preferred_element_type=jnp.float32,
        )
        * softmax_scale
    )
    allowed = usable[None, :] & (key_pos[None, :] <= query_position[:, None])
    scores = jnp.where(allowed[:, None, :], logits, -jnp.inf)
    maxima = lax.pmax(jnp.max(scores, axis=2), "ctx")
    weights = jnp.exp(scores - maxima[:, :, None])
    totals = jnp.sum(weights, axis=2)
    latent_mix = jnp.einsum(
        "qhk,kd->qhd",
        weights.astype(jnp.bfloat16),
        latent[:, :LAT_NOPE],
        preferred_element_type=jnp.float32,
    ).astype(jnp.bfloat16)
    values = jnp.einsum("qhd,hdv->qhv", latent_mix, value_up, preferred_element_type=jnp.float32)
    queries, head_count, value_width = values.shape
    numerators = values.reshape(queries, head_count * value_width)
    own_rows = query_latent.shape[0]
    numer_sum, denom_sum = lax.psum((numerators, totals), "ctx")
    attn_all = (
        (numer_sum.reshape(queries, head_count, value_width) / denom_sum[:, :, None])
        .reshape(queries, head_count * value_width)
        .astype(jnp.bfloat16)
    )
    attn_home = lax.dynamic_slice_in_dim(attn_all, shard_index * own_rows, own_rows, 0)
    summed = lax.psum_scatter(
        jnp.dot(attn_all, out_codes, preferred_element_type=jnp.float32),
        "head",
        scatter_dimension=0,
        tiled=True,
    )
    projected = (summed * out_scales[None, :]).astype(jnp.bfloat16)
    return (attn_home, projected)


def flip(index, mask):
    bit, result = 1, index
    while bit <= mask:
        if mask & bit:
            result = result + bit - 2 * bit * lax.rem(index // bit, 2)
        bit *= 2
    return result


def fused(
    n,
    heads,
    valid_hbm,
    qpos_hbm,
    query_hbm,
    codes_hbm,
    scales_hbm,
    up_hbm,
    out_hbm,
    attn_ref,
    proj_ref,
    valid,
    qpos,
    near_valid,
    q_all,
    codes,
    near_codes,
    scales,
    near_scales,
    up,
    outw,
    latent,
    mix,
    stat_m,
    stat_l,
    num_send,
    num_recv,
    st_send,
    st_recv,
    att_all,
    part,
    part_recv,
    sums,
    lent,
    lent_att,
    ready,
    in_sem,
    up_sem,
    out_sem,
    q_ssem,
    q_rsem,
    near_ssem,
    near_rsem,
    half_ssem,
    half_rsem,
    num_ssem,
    num_rsem,
    st_ssem,
    st_rsem,
    att_ssem,
    att_rsem,
    part_ssem,
    part_rsem,
    lent_ssem,
    lent_rsem,
):
    me = lax.axis_index("ctx")
    hd = lax.axis_index("head")
    other = 1 - hd
    row, column = me // 2, lax.rem(me, 2)
    rows = n // 2
    head_count, width = q_all.shape[1:]
    blocks, block, keys = codes.shape
    first = 3 * (blocks - 1) // 8
    units = [(b, min(2, first - b), 0) for b in range(0, first, 2)]
    units += [(b, min(2, blocks - 1 - b), 1) for b in range(first, blocks - 1, 2)]
    rest = pl.ds(blocks - 1, 1)
    nope = mix.shape[0] * LANES
    vhead = up.shape[2]
    twin = head_count // 2
    per = twin // rows
    lines = 2 * rows

    barrier = pltpu.get_barrier_semaphore()
    met = [1] + list(range(2, n, 2))

    def slot_of(k):
        return k if k < 2 else k // 2 + 1

    for k in met:
        later = flip(me, k)

        @pl.when(later > me)
        def _():
            pl.semaphore_signal(barrier, inc=1, device_id={"ctx": later}, device_id_type=MESH)

    @pl.when(hd == 0)
    def _():
        pl.semaphore_signal(barrier, inc=1, device_id={"head": other}, device_id_type=MESH)

    loads = [
        pltpu.make_async_copy(codes_hbm, codes, in_sem.at[0]),
        pltpu.make_async_copy(scales_hbm, scales, in_sem.at[1]),
        pltpu.make_async_copy(query_hbm.at[0], q_all.at[row], in_sem.at[2]),
        pltpu.make_async_copy(valid_hbm, valid, in_sem.at[3]),
        pltpu.make_async_copy(qpos_hbm, qpos, in_sem.at[4]),
    ]
    for copy in loads:
        copy.start()

    ahead = row + column + hd

    @pl.when(ahead > 0)
    def _():
        pl.semaphore_wait(barrier, ahead)

    @pl.when(hd == 1)
    def _():
        pl.semaphore_signal(ready.at[0], inc=1, device_id={"head": other}, device_id_type=MESH)

    for k in met:
        earlier = flip(me, k)

        @pl.when(earlier < me)
        def _():
            pl.semaphore_signal(ready.at[slot_of(k)], inc=1, device_id={"ctx": earlier}, device_id_type=MESH)

    def admit(k):
        @pl.when(flip(me, k) > me)
        def _():
            pl.semaphore_wait(ready.at[slot_of(k)], 1)

    def drain(ref, sem):
        pltpu.make_async_copy(ref, ref, sem).wait()

    def remote(src, dst, ssem, rsem, when=None, **device):
        copy = pltpu.make_async_remote_copy(
            src_ref=src,
            dst_ref=dst,
            send_sem=ssem,
            recv_sem=rsem,
            device_id=device,
            device_id_type=MESH,
        )
        copy.start() if when is None else pl.when(when)(copy.start)
        return copy

    for k in range(rows - 1, 0, -1):
        peer = flip(me, 2 * k)
        remote(query_hbm.at[0], q_all.at[row], q_ssem, q_rsem, peer < me, ctx=peer)

    admit(1)
    partner = flip(me, 1)
    near = [
        remote(valid_hbm, near_valid, near_ssem.at[0], near_rsem.at[0], ctx=partner),
        remote(scales_hbm, near_scales, near_ssem.at[1], near_rsem.at[1], hd == 1, ctx=partner),
    ]
    for p, (b, count, who) in enumerate(units):
        of = pl.ds(b, count)
        near.append(
            remote(
                codes_hbm.at[of],
                near_codes.at[of],
                near_ssem.at[2],
                near_rsem.at[2 + p],
                hd == who,
                ctx=partner,
            )
        )
    last = remote(
        codes_hbm.at[rest],
        near_codes.at[rest],
        near_ssem.at[3],
        near_rsem.at[2 + len(units)],
        ctx=partner,
    )

    up_in = pltpu.make_async_copy(up_hbm, up, up_sem)
    up_in.start()
    loads.pop(2).wait()
    for k in range(1, rows):
        admit(2 * k)
        peer = flip(me, 2 * k)
        remote(q_all.at[row], q_all.at[row], q_ssem, q_rsem, peer > me, ctx=peer)

    out_in = pltpu.make_async_copy(out_hbm, outw, out_sem)
    out_in.start()

    def scale_latent(source, factors, at, of):
        for b in of:
            latent[b * block : (b + 1) * block, at : at + keys] = (
                source[b].astype(jnp.float32) * factors[b : b + 1, :]
            ).astype(jnp.bfloat16)

    for copy in loads:
        copy.wait()
    scale_latent(codes, scales, 0, range(blocks))

    relayed = []

    def relay(ref, index, who):
        pl.when(hd == who)(near[index].wait_recv)
        relayed.append(
            remote(ref, ref, half_ssem.at[min(index, 2) - 1], half_rsem.at[index - 1], hd == who, head=other)
        )

    @pl.when(hd == 0)
    def _():
        pl.semaphore_wait(ready.at[0], 1)

    relay(near_scales, 1, 1)
    for p, (b, count, who) in enumerate(units):
        relay(near_codes.at[pl.ds(b, count)], 2 + p, who)
    pl.when(hd == 0)(relayed[0].wait_recv)
    near[0].wait_recv()
    for p, (b, count, who) in enumerate(units):
        pl.when(hd != who)(relayed[1 + p].wait_recv)
        scale_latent(near_codes, near_scales, keys, range(b, b + count))
    last.wait_recv()
    scale_latent(near_codes, near_scales, keys, range(blocks - 1, blocks))
    drain(q_all.at[pl.ds(0, rows - 1)], q_rsem)
    logits = jnp.dot(
        q_all[...].reshape(rows * head_count, width), latent[...], preferred_element_type=jnp.float32
    )
    slot = lax.broadcasted_iota(jnp.int32, (head_count, 2 * keys), 1)
    weights = []
    for t in range(rows):
        position = qpos[2 * t + column]
        own_limit = jnp.minimum(valid[0], position - me * keys + 1)
        near_limit = jnp.minimum(near_valid[0], position - partner * keys + 1)
        allowed = slot < jnp.where(slot < keys, own_limit, near_limit + keys)
        of = slice(t * head_count, (t + 1) * head_count)
        scores = jnp.where(allowed, logits[of], MASKED)
        top = jnp.maximum(jnp.max(scores, axis=1, keepdims=True), FLOOR)
        weight = jnp.exp2((scores - top) * EXPONENT)
        stat_m[of, :] = jnp.broadcast_to(top, (head_count, LANES))
        stat_l[of, :] = jnp.broadcast_to(jnp.sum(weight, axis=1, keepdims=True), (head_count, LANES))
        weights.append(weight.astype(jnp.bfloat16))
    mixed_all = lax.dot_general(
        jnp.concatenate(weights, axis=0),
        latent[:nope, :],
        (((1,), (1,)), ((), ())),
        preferred_element_type=jnp.float32,
    )
    for c in range(mix.shape[0]):
        mix[c] = mixed_all[:, c * LANES : (c + 1) * LANES]

    up_in.wait()
    tile_lane = lax.broadcasted_iota(jnp.int32, (lines, LANES), 1)
    even = lax.rem(lax.broadcasted_iota(jnp.int32, (lines, LANES), 0), 2) == 0
    for k in range(rows - 1, -1, -1):
        group = flip(row, k)
        stat = jnp.zeros((lines, LANES), jnp.float32)
        for j in range(per):
            of = pl.ds(group * per + j, lines, stride=twin)
            stat = jnp.where(tile_lane == j, stat_m[of, :], stat)
            stat = jnp.where(tile_lane == per + j, stat_l[of, :], stat)
        st_send[k] = stat
        if k:
            remote(st_send.at[k], st_recv.at[k], st_ssem, st_rsem, ctx=flip(me, 2 * k))
        for j in range(per):
            h = group * per + j
            of = pl.ds(h, lines, stride=twin)
            mixed = jnp.concatenate(
                [mix[c, of, :] for c in range(mix.shape[0])], axis=1
            ).astype(jnp.bfloat16)
            pair = jnp.dot(
                mixed,
                jnp.concatenate([up[h], up[h + twin]], axis=1),
                preferred_element_type=jnp.float32,
            )
            num_send[k, j] = jnp.where(even, pair[:, :vhead], pair[:, vhead:]).astype(jnp.bfloat16)
        if k:
            remote(num_send.at[k], num_recv.at[k], num_ssem, num_rsem, ctx=flip(me, 2 * k))

    @pl.when(hd == 0)
    def _():
        for p in range(2):
            at = (p * twin + flip(row, rows - 1) * per) * vhead
            remote(
                out_hbm.at[pl.ds(pl.multiple_of(at, per * vhead), per * vhead)],
                lent.at[p],
                lent_ssem.at[0],
                lent_rsem.at[0],
                head=other,
            )

    drain(st_recv.at[pl.ds(1, rows - 1)], st_rsem)
    stats = [st_send[0]] + [st_recv[k] for k in range(1, rows)]
    top = functools.reduce(jnp.maximum, stats)
    factors = [jnp.exp2((s - top) * EXPONENT) for s in stats]
    shares = []
    for j in range(per):
        total = sum(f[:, j : j + 1] * s[:, per + j : per + j + 1] for s, f in zip(stats, factors))
        shares.append([jnp.broadcast_to(f[:, j : j + 1] / total, (lines, vhead)) for f in factors])
    drain(num_recv.at[pl.ds(1, rows - 1)], num_rsem)
    for j in range(per):
        value = shares[j][0] * num_send[0, j].astype(jnp.float32)
        for k in range(1, rows):
            value += shares[j][k] * num_recv[k, j].astype(jnp.float32)
        att_all[me, j] = value.astype(jnp.bfloat16)

    @pl.when(hd == 0)
    def _():
        for target in (flip(me, n - 1), flip(me, n - 2)):
            remote(
                att_all.at[me],
                lent_att.at[column],
                lent_ssem.at[1],
                lent_rsem.at[1],
                ctx=target,
                head=other,
            )

    for k in range(n - 1, 0, -1):
        remote(
            att_all.at[me],
            att_all.at[me],
            att_ssem,
            att_rsem.at[k // 2],
            None if k < n - 1 else hd == 1,
            ctx=flip(me, k),
        )

    for copy in [near[0], last]:
        copy.wait_send()
    drain(q_all.at[pl.ds(0, rows - 1)], q_ssem)
    drain(st_send.at[pl.ds(1, rows - 1)], st_ssem)
    drain(num_send.at[pl.ds(1, rows - 1)], num_ssem)

    @pl.when(hd == 0)
    def _():
        ours = near_codes.at[pl.ds(0, first)]
        drain(ours, near_ssem.at[2])
        drain(ours, half_ssem.at[1])

    @pl.when(hd == 1)
    def _():
        ours = near_codes.at[pl.ds(first, blocks - 1 - first)]
        drain(near_scales, near_ssem.at[1])
        drain(near_scales, half_ssem.at[0])
        drain(ours, near_ssem.at[2])
        drain(ours, half_ssem.at[1])

    out_in.wait()
    columns = outw.shape[1]
    acc = jnp.zeros((2 * lines, columns), jnp.float32)
    both = lax.rem(lax.broadcasted_iota(jnp.int32, (2 * lines, LANES), 0), 2) == 0
    own_line = lax.broadcasted_iota(jnp.int32, (lines, LANES), 0)

    def keep(group):
        for j in range(per):
            tile = att_all[2 * group + column, j].astype(jnp.float32)
            for p in range(2):
                at = pl.multiple_of((p * twin + group * per + j) * vhead, vhead)
                attn_ref[:, pl.ds(at, vhead)] = jnp.sum(
                    jnp.where(own_line == 2 * row + p, tile, 0.0), axis=0, keepdims=True
                )

    def product(piece, weight):
        evens, odds = [], []
        for j in range(per):
            tile = jnp.concatenate([piece(c, j).astype(jnp.float32) for c in range(2)], axis=0)
            evens.append(jnp.where(both, tile, 0.0).astype(jnp.bfloat16))
            odds.append(jnp.where(both, 0.0, tile).astype(jnp.bfloat16))
        out = jnp.zeros((2 * lines, columns), jnp.float32)
        for p, side in enumerate((evens, odds)):
            left = jnp.concatenate(side, axis=1)
            cuts = (0, LANES, columns) if p else (0, columns)
            out += jnp.concatenate(
                [
                    jnp.dot(left, weight(p, low, high), preferred_element_type=jnp.float32)
                    for low, high in zip(cuts, cuts[1:])
                ],
                axis=1,
            )
        return out

    def arrive(k, count=2):
        drain(att_all.at[pl.ds(0, count if k else 1)], att_rsem.at[k])

    def project(k):
        group = flip(row, k)
        arrive(k)

        def weight(p, low, high):
            at = pl.multiple_of((p * twin + group * per) * vhead, per * vhead)
            return outw[pl.ds(at, per * vhead), low:high]

        return product(lambda c, j: att_all[2 * group + c, j], weight)

    for k in range(rows - 1):
        acc += project(k)
        if k < rows - 2:
            keep(flip(row, k))
    sums[...] = acc

    @pl.when(hd == 1)
    def _():
        sums[...] += project(rows - 1)
        drain(lent, lent_rsem.at[0])
        drain(lent_att, lent_rsem.at[1])
        sums[...] += product(lambda c, j: lent_att[c, j], lambda p, low, high: lent[p, :, low:high])

    acc = sums[...]
    share = n // heads
    for i in range(heads):
        lots = []
        for token in range(i * share, (i + 1) * share):
            at = token % 2 * lines + token // 2 * 2
            lots.append(acc[at : at + 1] + acc[at + 1 : at + 2])
        part[i] = jnp.concatenate(lots, axis=0)
    swap = remote(part.at[other], part_recv, part_ssem, part_rsem, head=other)
    pl.when(hd == 0)(lambda: arrive(rows - 1, 1))
    for k in (rows - 2, rows - 1):
        keep(flip(row, k))
    swap.wait_recv()
    proj_ref[...] = part[hd] + part_recv[...]
    drain(att_all.at[pl.ds(0, n - 2)], att_ssem)

    @pl.when(hd == 0)
    def _():
        drain(lent, lent_ssem.at[0])
        drain(lent_att, lent_ssem.at[1])

    pl.when(hd == 1)(lambda: drain(att_all.at[pl.ds(0, 1)], att_ssem))
    swap.wait_send()


def finish(attn_ref, summed_ref, scales_ref, attn_out, proj_out):
    attn_out[...] = attn_ref[...].astype(jnp.bfloat16)
    proj_out[...] = (summed_ref[...] * scales_ref[...].reshape(1, -1)).astype(jnp.bfloat16)


def block(n, heads, *args):
    query, codes, scales, valid, qpos, up, outw, out_scales = args
    own, head_count, width = query.shape
    keys, blocks = scales.shape
    chunk = blocks // 2 + 5
    fits = own == 1 and heads == 2 and n >= 4 and n & (n - 1) == 0 and head_count % n == 0
    fits = fits and width % blocks == 0 and width // blocks % 16 == 0 and blocks > 8
    if not fits:
        return shards(*args)
    vhead = up.shape[2]
    rows, lines = n // 2, n
    per = head_count // n
    columns = outw.shape[1]
    anywhere = pl.BlockSpec(memory_space=pltpu.HBM)
    vmem = pl.BlockSpec(memory_space=pltpu.VMEM)
    dma = pltpu.SemaphoreType.DMA
    attention, summed = pl.pallas_call(
        functools.partial(fused, n, heads),
        out_shape=(
            jax.ShapeDtypeStruct((own, head_count * vhead), jnp.float32),
            jax.ShapeDtypeStruct((n // heads, columns), jnp.float32),
        ),
        in_specs=[anywhere] * 7,
        out_specs=(vmem, vmem),
        scratch_shapes=[
            pltpu.SMEM(valid.shape, jnp.int32),
            pltpu.SMEM(qpos.shape, jnp.int32),
            pltpu.SMEM(valid.shape, jnp.int32),
            pltpu.VMEM((rows, head_count, width), jnp.bfloat16),
            pltpu.VMEM((blocks, width // blocks, keys), jnp.bfloat16),
            pltpu.VMEM((blocks, width // blocks, keys), jnp.bfloat16),
            pltpu.VMEM((blocks, keys), jnp.float32),
            pltpu.VMEM((blocks, keys), jnp.float32),
            pltpu.VMEM(up.shape, jnp.bfloat16),
            pltpu.VMEM(outw.shape, jnp.bfloat16),
            pltpu.VMEM((width, 2 * keys), jnp.bfloat16),
            pltpu.VMEM((LAT_NOPE // LANES, rows * head_count, LANES), jnp.float32),
            pltpu.VMEM((rows * head_count, LANES), jnp.float32),
            pltpu.VMEM((rows * head_count, LANES), jnp.float32),
            pltpu.VMEM((rows, per, lines, vhead), jnp.bfloat16),
            pltpu.VMEM((rows, per, lines, vhead), jnp.bfloat16),
            pltpu.VMEM((rows, lines, LANES), jnp.float32),
            pltpu.VMEM((rows, lines, LANES), jnp.float32),
            pltpu.VMEM((n, per, lines, vhead), jnp.bfloat16),
            pltpu.VMEM((heads, n // heads, columns), jnp.float32),
            pltpu.VMEM((n // heads, columns), jnp.float32),
            pltpu.VMEM((n * 2, columns), jnp.float32),
            pltpu.VMEM((2, per * vhead, columns), jnp.bfloat16),
            pltpu.VMEM((2, per, lines, vhead), jnp.bfloat16),
            pltpu.SemaphoreType.REGULAR((rows + 1,)),
            dma((5,)),
            dma,
            dma,
            dma,
            dma,
            dma((4,)),
            dma((chunk,)),
            dma((2,)),
            dma((chunk - 2,)),
            dma,
            dma,
            dma,
            dma,
            dma,
            dma((rows,)),
            dma,
            dma,
            dma((2,)),
            dma((2,)),
        ],
        compiler_params=pltpu.CompilerParams(
            collective_id=0, has_side_effects=True, vmem_limit_bytes=32 * 1024 * 1024
        ),
        name="mla_block",
    )(
        valid,
        *(
            pltpu.with_memory_space_constraint(operand, pltpu.HBM)
            for operand in (
                qpos,
                query,
                codes.T.reshape(blocks, width // blocks, keys),
                scales.T,
                up,
                outw,
            )
        ),
    )
    return pl.pallas_call(
        finish,
        out_shape=(
            jax.ShapeDtypeStruct((own, head_count * vhead), jnp.bfloat16),
            jax.ShapeDtypeStruct((n // heads, columns), jnp.bfloat16),
        ),
        in_specs=[vmem] * 3,
        out_specs=(vmem, vmem),
        compiler_params=pltpu.CompilerParams(vmem_limit_bytes=1024 * 1024),
        name="finish",
    )(attention, summed, out_scales)


def solution(mesh):
    ctx, heads = mesh.shape["ctx"], mesh.shape["head"]
    return jax.shard_map(
        functools.partial(block, ctx, heads),
        mesh=mesh,
        in_specs=(
            P(("groups", "ctx"), "head", None),
            P(("groups", "ctx"), None),
            P(("groups", "ctx"), None),
            P(("groups", "ctx")),
            P("groups"),
            P("head", None, None),
            P("head", "ctx"),
            P("ctx"),
        ),
        out_specs=(P(("groups", "ctx"), "head"), P(("groups", "head"), "ctx")),
        check_vma=False,
    )
```

```python
import functools
import math

import jax
import jax.numpy as jnp
from jax import lax
from jax.experimental import pallas as pl
from jax.experimental.pallas import tpu as pltpu
from jax.sharding import PartitionSpec as P

LAT_NOPE = 512
ROPE = 64
QK_NOPE = 128
LANES = 128
MASKED = -1e30
FLOOR = -1e29
EXPONENT = math.log2(math.e) * (QK_NOPE + ROPE) ** -0.5
MESH = pl.DeviceIdType.MESH


def shards(
    query_latent,
    latent_codes,
    latent_scales,
    valid_lengths,
    query_position,
    value_up,
    out_codes,
    out_scales,
):
    key_count, width = latent_codes.shape
    block_count = latent_scales.shape[1]
    latent = (
        (
            latent_codes.astype(jnp.float32).reshape(key_count, block_count, width // block_count)
            * latent_scales[:, :, None]
        )
        .reshape(key_count, width)
        .astype(jnp.bfloat16)
    )
    shard_index = lax.axis_index("ctx")
    local_slots = jnp.arange(key_count, dtype=jnp.int32)
    key_pos = shard_index * key_count + local_slots
    usable = local_slots < valid_lengths[0]
    softmax_scale = (QK_NOPE + ROPE) ** (-0.5)
    logits = (
        jnp.einsum(
            "qhc,kc->qhk",
            lax.all_gather(query_latent, "ctx", axis=0, tiled=True),
            latent,
            preferred_element_type=jnp.float32,
        )
        * softmax_scale
    )
    allowed = usable[None, :] & (key_pos[None, :] <= query_position[:, None])
    scores = jnp.where(allowed[:, None, :], logits, -jnp.inf)
    maxima = lax.pmax(jnp.max(scores, axis=2), "ctx")
    weights = jnp.exp(scores - maxima[:, :, None])
    totals = jnp.sum(weights, axis=2)
    latent_mix = jnp.einsum(
        "qhk,kd->qhd",
        weights.astype(jnp.bfloat16),
        latent[:, :LAT_NOPE],
        preferred_element_type=jnp.float32,
    ).astype(jnp.bfloat16)
    values = jnp.einsum("qhd,hdv->qhv", latent_mix, value_up, preferred_element_type=jnp.float32)
    queries, head_count, value_width = values.shape
    numerators = values.reshape(queries, head_count * value_width)
    own_rows = query_latent.shape[0]
    numer_sum, denom_sum = lax.psum((numerators, totals), "ctx")
    attn_all = (
        (numer_sum.reshape(queries, head_count, value_width) / denom_sum[:, :, None])
        .reshape(queries, head_count * value_width)
        .astype(jnp.bfloat16)
    )
    attn_home = lax.dynamic_slice_in_dim(attn_all, shard_index * own_rows, own_rows, 0)
    summed = lax.psum_scatter(
        jnp.dot(attn_all, out_codes, preferred_element_type=jnp.float32),
        "head",
        scatter_dimension=0,
        tiled=True,
    )
    projected = (summed * out_scales[None, :]).astype(jnp.bfloat16)
    return (attn_home, projected)


def flip(index, mask):
    bit, result = 1, index
    while bit <= mask:
        if mask & bit:
            result = result + bit - 2 * bit * lax.rem(index // bit, 2)
        bit *= 2
    return result


def fused(
    n,
    heads,
    valid_hbm,
    qpos_hbm,
    query_hbm,
    codes_hbm,
    scales_hbm,
    up_hbm,
    out_hbm,
    attn_ref,
    proj_ref,
    valid,
    qpos,
    near_valid,
    q_all,
    codes,
    near_codes,
    scales,
    near_scales,
    up,
    outw,
    latent,
    mix,
    stat_m,
    stat_l,
    num_send,
    num_recv,
    st_send,
    st_recv,
    att_all,
    part,
    part_recv,
    sums,
    lent,
    lent_att,
    ready,
    in_sem,
    up_sem,
    out_sem,
    q_ssem,
    q_rsem,
    near_ssem,
    near_rsem,
    half_ssem,
    half_rsem,
    num_ssem,
    num_rsem,
    st_ssem,
    st_rsem,
    att_ssem,
    att_rsem,
    part_ssem,
    part_rsem,
    lent_ssem,
    lent_rsem,
):
    me = lax.axis_index("ctx")
    hd = lax.axis_index("head")
    other = 1 - hd
    row, column = me // 2, lax.rem(me, 2)
    rows = n // 2
    head_count, width = q_all.shape[1:]
    blocks, block, keys = codes.shape
    first = 3 * (blocks - 1) // 8
    units = [(b, min(2, first - b), 0, b // 2) for b in range(0, first, 2)]
    units += [
        (b, min(2, blocks - 1 - b), 1, (b - first) // 2) for b in range(first, blocks - 1, 2)
    ]
    turns = near_rsem.shape[0] - 3
    rest = pl.ds(blocks - 1, 1)
    nope = mix.shape[0] * LANES
    vhead = up.shape[2]
    twin = head_count // 2
    per = twin // rows
    lines = 2 * rows

    barrier = pltpu.get_barrier_semaphore()
    met = [1] + list(range(2, n, 2))

    def slot_of(k):
        return k if k < 2 else k // 2 + 1

    for k in met:
        later = flip(me, k)

        @pl.when(later > me)
        def _():
            pl.semaphore_signal(barrier, inc=1, device_id={"ctx": later}, device_id_type=MESH)

    @pl.when(hd == 0)
    def _():
        pl.semaphore_signal(barrier, inc=1, device_id={"head": other}, device_id_type=MESH)

    loads = [
        pltpu.make_async_copy(codes_hbm, codes, in_sem.at[0]),
        pltpu.make_async_copy(scales_hbm, scales, in_sem.at[1]),
        pltpu.make_async_copy(query_hbm.at[0], q_all.at[row], in_sem.at[2]),
        pltpu.make_async_copy(valid_hbm, valid, in_sem.at[3]),
        pltpu.make_async_copy(qpos_hbm, qpos, in_sem.at[4]),
    ]
    for copy in loads:
        copy.start()

    ahead = row + column + hd

    @pl.when(ahead > 0)
    def _():
        pl.semaphore_wait(barrier, ahead)

    @pl.when(hd == 1)
    def _():
        pl.semaphore_signal(ready.at[0], inc=1, device_id={"head": other}, device_id_type=MESH)

    for k in met:
        earlier = flip(me, k)

        @pl.when(earlier < me)
        def _():
            pl.semaphore_signal(ready.at[slot_of(k)], inc=1, device_id={"ctx": earlier}, device_id_type=MESH)

    def admit(k):
        @pl.when(flip(me, k) > me)
        def _():
            pl.semaphore_wait(ready.at[slot_of(k)], 1)

    def drain(ref, sem):
        pltpu.make_async_copy(ref, ref, sem).wait()

    def remote(src, dst, ssem, rsem, when=None, **device):
        copy = pltpu.make_async_remote_copy(
            src_ref=src,
            dst_ref=dst,
            send_sem=ssem,
            recv_sem=rsem,
            device_id=device,
            device_id_type=MESH,
        )
        copy.start() if when is None else pl.when(when)(copy.start)
        return copy

    for k in range(rows - 1, 0, -1):
        peer = flip(me, 2 * k)
        remote(query_hbm.at[0], q_all.at[row], q_ssem, q_rsem, peer < me, ctx=peer)

    admit(1)
    partner = flip(me, 1)
    near = [
        remote(valid_hbm, near_valid, near_ssem.at[0], near_rsem.at[0], ctx=partner),
        remote(scales_hbm, near_scales, near_ssem.at[1], near_rsem.at[1], hd == 1, ctx=partner),
    ]
    for b, count, who, turn in units:
        of = pl.ds(b, count)
        near.append(
            remote(
                codes_hbm.at[of],
                near_codes.at[of],
                near_ssem.at[2],
                near_rsem.at[2 + turn],
                hd == who,
                ctx=partner,
            )
        )
    last = remote(
        codes_hbm.at[rest],
        near_codes.at[rest],
        near_ssem.at[3],
        near_rsem.at[2 + turns],
        ctx=partner,
    )

    up_in = pltpu.make_async_copy(up_hbm, up, up_sem)
    up_in.start()
    loads.pop(2).wait()
    for k in range(1, rows):
        admit(2 * k)
        peer = flip(me, 2 * k)
        remote(q_all.at[row], q_all.at[row], q_ssem, q_rsem, peer > me, ctx=peer)

    out_in = pltpu.make_async_copy(out_hbm, outw, out_sem)
    out_in.start()

    def scale_latent(source, factors, at, of):
        for b in of:
            latent[b * block : (b + 1) * block, at : at + keys] = (
                source[b].astype(jnp.float32) * factors[b : b + 1, :]
            ).astype(jnp.bfloat16)

    for copy in loads:
        copy.wait()
    scale_latent(codes, scales, 0, range(blocks))

    relayed = []

    def relay(ref, index, turn, who):
        pl.when(hd == who)(near[index].wait_recv)
        relayed.append(
            remote(ref, ref, half_ssem.at[min(index, 2) - 1], half_rsem.at[turn], hd == who, head=other)
        )

    @pl.when(hd == 0)
    def _():
        pl.semaphore_wait(ready.at[0], 1)

    relay(near_scales, 1, 0, 1)
    for p, (b, count, who, turn) in enumerate(units):
        relay(near_codes.at[pl.ds(b, count)], 2 + p, 1 + turn, who)
    pl.when(hd == 0)(relayed[0].wait_recv)
    near[0].wait_recv()
    for p, (b, count, who, _) in enumerate(units):
        pl.when(hd != who)(relayed[1 + p].wait_recv)
        scale_latent(near_codes, near_scales, keys, range(b, b + count))
    last.wait_recv()
    scale_latent(near_codes, near_scales, keys, range(blocks - 1, blocks))
    drain(q_all.at[pl.ds(0, rows - 1)], q_rsem)
    logits = jnp.dot(
        q_all[...].reshape(rows * head_count, width), latent[...], preferred_element_type=jnp.float32
    )
    slot = lax.broadcasted_iota(jnp.int32, (head_count, 2 * keys), 1)
    weights = []
    for t in range(rows):
        position = qpos[2 * t + column]
        own_limit = jnp.minimum(valid[0], position - me * keys + 1)
        near_limit = jnp.minimum(near_valid[0], position - partner * keys + 1)
        allowed = slot < jnp.where(slot < keys, own_limit, near_limit + keys)
        of = slice(t * head_count, (t + 1) * head_count)
        scores = jnp.where(allowed, logits[of], MASKED)
        top = jnp.maximum(jnp.max(scores, axis=1, keepdims=True), FLOOR)
        weight = jnp.exp2((scores - top) * EXPONENT)
        stat_m[of, :] = jnp.broadcast_to(top, (head_count, LANES))
        stat_l[of, :] = jnp.broadcast_to(jnp.sum(weight, axis=1, keepdims=True), (head_count, LANES))
        weights.append(weight.astype(jnp.bfloat16))
    mixed_all = lax.dot_general(
        jnp.concatenate(weights, axis=0),
        latent[:nope, :],
        (((1,), (1,)), ((), ())),
        preferred_element_type=jnp.float32,
    )
    for c in range(mix.shape[0]):
        mix[c] = mixed_all[:, c * LANES : (c + 1) * LANES]

    up_in.wait()
    tile_lane = lax.broadcasted_iota(jnp.int32, (lines, LANES), 1)
    even = lax.rem(lax.broadcasted_iota(jnp.int32, (lines, LANES), 0), 2) == 0
    for k in range(rows - 1, -1, -1):
        group = flip(row, k)
        stat = jnp.zeros((lines, LANES), jnp.float32)
        for j in range(per):
            of = pl.ds(group * per + j, lines, stride=twin)
            stat = jnp.where(tile_lane == j, stat_m[of, :], stat)
            stat = jnp.where(tile_lane == per + j, stat_l[of, :], stat)
        st_send[k] = stat
        if k:
            remote(st_send.at[k], st_recv.at[k], st_ssem, st_rsem, ctx=flip(me, 2 * k))
        for j in range(per):
            h = group * per + j
            of = pl.ds(h, lines, stride=twin)
            mixed = jnp.concatenate(
                [mix[c, of, :] for c in range(mix.shape[0])], axis=1
            ).astype(jnp.bfloat16)
            pair = jnp.dot(
                mixed,
                jnp.concatenate([up[h], up[h + twin]], axis=1),
                preferred_element_type=jnp.float32,
            )
            num_send[k, j] = jnp.where(even, pair[:, :vhead], pair[:, vhead:]).astype(jnp.bfloat16)
        if k:
            remote(num_send.at[k], num_recv.at[k], num_ssem, num_rsem, ctx=flip(me, 2 * k))

    @pl.when(hd == 0)
    def _():
        for p in range(2):
            at = (p * twin + flip(row, rows - 1) * per) * vhead
            remote(
                out_hbm.at[pl.ds(pl.multiple_of(at, per * vhead), per * vhead)],
                lent.at[p],
                lent_ssem.at[0],
                lent_rsem.at[0],
                head=other,
            )

    drain(st_recv.at[pl.ds(1, rows - 1)], st_rsem)
    stats = [st_send[0]] + [st_recv[k] for k in range(1, rows)]
    top = functools.reduce(jnp.maximum, stats)
    factors = [jnp.exp2((s - top) * EXPONENT) for s in stats]
    shares = []
    for j in range(per):
        total = sum(f[:, j : j + 1] * s[:, per + j : per + j + 1] for s, f in zip(stats, factors))
        shares.append([jnp.broadcast_to(f[:, j : j + 1] / total, (lines, vhead)) for f in factors])
    drain(num_recv.at[pl.ds(1, rows - 1)], num_rsem)
    for j in range(per):
        value = shares[j][0] * num_send[0, j].astype(jnp.float32)
        for k in range(1, rows):
            value += shares[j][k] * num_recv[k, j].astype(jnp.float32)
        att_all[me, j] = value.astype(jnp.bfloat16)

    @pl.when(hd == 0)
    def _():
        for target in (flip(me, n - 1), flip(me, n - 2)):
            remote(
                att_all.at[me],
                lent_att.at[column],
                lent_ssem.at[1],
                lent_rsem.at[1],
                ctx=target,
                head=other,
            )

    for k in range(n - 1, 0, -1):
        remote(
            att_all.at[me],
            att_all.at[me],
            att_ssem,
            att_rsem.at[k // 2],
            None if k < n - 1 else hd == 1,
            ctx=flip(me, k),
        )

    for copy in [near[0], last]:
        copy.wait_send()
    drain(q_all.at[pl.ds(0, rows - 1)], q_ssem)
    drain(st_send.at[pl.ds(1, rows - 1)], st_ssem)
    drain(num_send.at[pl.ds(1, rows - 1)], num_ssem)

    @pl.when(hd == 0)
    def _():
        ours = near_codes.at[pl.ds(0, first)]
        drain(ours, near_ssem.at[2])
        drain(ours, half_ssem.at[1])

    @pl.when(hd == 1)
    def _():
        ours = near_codes.at[pl.ds(first, blocks - 1 - first)]
        drain(near_scales, near_ssem.at[1])
        drain(near_scales, half_ssem.at[0])
        drain(ours, near_ssem.at[2])
        drain(ours, half_ssem.at[1])

    out_in.wait()
    columns = outw.shape[1]
    acc = jnp.zeros((2 * lines, columns), jnp.float32)
    both = lax.rem(lax.broadcasted_iota(jnp.int32, (2 * lines, LANES), 0), 2) == 0
    own_line = lax.broadcasted_iota(jnp.int32, (lines, LANES), 0)

    def keep(group):
        for j in range(per):
            tile = att_all[2 * group + column, j].astype(jnp.float32)
            for p in range(2):
                at = pl.multiple_of((p * twin + group * per + j) * vhead, vhead)
                attn_ref[:, pl.ds(at, vhead)] = jnp.sum(
                    jnp.where(own_line == 2 * row + p, tile, 0.0), axis=0, keepdims=True
                )

    def product(piece, weight):
        evens, odds = [], []
        for j in range(per):
            tile = jnp.concatenate([piece(c, j).astype(jnp.float32) for c in range(2)], axis=0)
            evens.append(jnp.where(both, tile, 0.0).astype(jnp.bfloat16))
            odds.append(jnp.where(both, 0.0, tile).astype(jnp.bfloat16))
        out = jnp.zeros((2 * lines, columns), jnp.float32)
        for p, side in enumerate((evens, odds)):
            left = jnp.concatenate(side, axis=1)
            cuts = (0, LANES, columns) if p else (0, columns)
            out += jnp.concatenate(
                [
                    jnp.dot(left, weight(p, low, high), preferred_element_type=jnp.float32)
                    for low, high in zip(cuts, cuts[1:])
                ],
                axis=1,
            )
        return out

    def arrive(k, count=2):
        drain(att_all.at[pl.ds(0, count if k else 1)], att_rsem.at[k])

    def project(k):
        group = flip(row, k)
        arrive(k)

        def weight(p, low, high):
            at = pl.multiple_of((p * twin + group * per) * vhead, per * vhead)
            return outw[pl.ds(at, per * vhead), low:high]

        return product(lambda c, j: att_all[2 * group + c, j], weight)

    for k in range(rows - 1):
        acc += project(k)
        if k < rows - 2:
            keep(flip(row, k))
    sums[...] = acc

    @pl.when(hd == 1)
    def _():
        sums[...] += project(rows - 1)
        drain(lent, lent_rsem.at[0])
        drain(lent_att, lent_rsem.at[1])
        sums[...] += product(lambda c, j: lent_att[c, j], lambda p, low, high: lent[p, :, low:high])

    acc = sums[...]
    share = n // heads
    for i in range(heads):
        lots = []
        for token in range(i * share, (i + 1) * share):
            at = token % 2 * lines + token // 2 * 2
            lots.append(acc[at : at + 1] + acc[at + 1 : at + 2])
        part[i] = jnp.concatenate(lots, axis=0)
    swap = remote(part.at[other], part_recv, part_ssem, part_rsem, head=other)
    pl.when(hd == 0)(lambda: arrive(rows - 1, 1))
    for k in (rows - 2, rows - 1):
        keep(flip(row, k))
    swap.wait_recv()
    proj_ref[...] = part[hd] + part_recv[...]
    drain(att_all.at[pl.ds(0, n - 2)], att_ssem)

    @pl.when(hd == 0)
    def _():
        drain(lent, lent_ssem.at[0])
        drain(lent_att, lent_ssem.at[1])

    pl.when(hd == 1)(lambda: drain(att_all.at[pl.ds(0, 1)], att_ssem))
    swap.wait_send()


def finish(attn_ref, summed_ref, scales_ref, attn_out, proj_out):
    attn_out[...] = attn_ref[...].astype(jnp.bfloat16)
    proj_out[...] = (summed_ref[...] * scales_ref[...].reshape(1, -1)).astype(jnp.bfloat16)


def block(n, heads, *args):
    query, codes, scales, valid, qpos, up, outw, out_scales = args
    own, head_count, width = query.shape
    keys, blocks = scales.shape
    turns = (5 * (blocks - 1) // 8 + 2) // 2
    fits = own == 1 and heads == 2 and n >= 4 and n & (n - 1) == 0 and head_count % n == 0
    fits = fits and width % blocks == 0 and width // blocks % 16 == 0 and blocks > 8
    if not fits:
        return shards(*args)
    vhead = up.shape[2]
    rows, lines = n // 2, n
    per = head_count // n
    columns = outw.shape[1]
    anywhere = pl.BlockSpec(memory_space=pltpu.HBM)
    vmem = pl.BlockSpec(memory_space=pltpu.VMEM)
    dma = pltpu.SemaphoreType.DMA
    attention, summed = pl.pallas_call(
        functools.partial(fused, n, heads),
        out_shape=(
            jax.ShapeDtypeStruct((own, head_count * vhead), jnp.float32),
            jax.ShapeDtypeStruct((n // heads, columns), jnp.float32),
        ),
        in_specs=[anywhere] * 7,
        out_specs=(vmem, vmem),
        scratch_shapes=[
            pltpu.SMEM(valid.shape, jnp.int32),
            pltpu.SMEM(qpos.shape, jnp.int32),
            pltpu.SMEM(valid.shape, jnp.int32),
            pltpu.VMEM((rows, head_count, width), jnp.bfloat16),
            pltpu.VMEM((blocks, width // blocks, keys), jnp.bfloat16),
            pltpu.VMEM((blocks, width // blocks, keys), jnp.bfloat16),
            pltpu.VMEM((blocks, keys), jnp.float32),
            pltpu.VMEM((blocks, keys), jnp.float32),
            pltpu.VMEM(up.shape, jnp.bfloat16),
            pltpu.VMEM(outw.shape, jnp.bfloat16),
            pltpu.VMEM((width, 2 * keys), jnp.bfloat16),
            pltpu.VMEM((LAT_NOPE // LANES, rows * head_count, LANES), jnp.float32),
            pltpu.VMEM((rows * head_count, LANES), jnp.float32),
            pltpu.VMEM((rows * head_count, LANES), jnp.float32),
            pltpu.VMEM((rows, per, lines, vhead), jnp.bfloat16),
            pltpu.VMEM((rows, per, lines, vhead), jnp.bfloat16),
            pltpu.VMEM((rows, lines, LANES), jnp.float32),
            pltpu.VMEM((rows, lines, LANES), jnp.float32),
            pltpu.VMEM((n, per, lines, vhead), jnp.bfloat16),
            pltpu.VMEM((heads, n // heads, columns), jnp.float32),
            pltpu.VMEM((n // heads, columns), jnp.float32),
            pltpu.VMEM((n * 2, columns), jnp.float32),
            pltpu.VMEM((2, per * vhead, columns), jnp.bfloat16),
            pltpu.VMEM((2, per, lines, vhead), jnp.bfloat16),
            pltpu.SemaphoreType.REGULAR((rows + 1,)),
            dma((5,)),
            dma,
            dma,
            dma,
            dma,
            dma((4,)),
            dma((3 + turns,)),
            dma((2,)),
            dma((1 + turns,)),
            dma,
            dma,
            dma,
            dma,
            dma,
            dma((rows,)),
            dma,
            dma,
            dma((2,)),
            dma((2,)),
        ],
        compiler_params=pltpu.CompilerParams(
            collective_id=0, has_side_effects=True, vmem_limit_bytes=32 * 1024 * 1024
        ),
        name="mla_block",
    )(
        valid,
        *(
            pltpu.with_memory_space_constraint(operand, pltpu.HBM)
            for operand in (
                qpos,
                query,
                codes.T.reshape(blocks, width // blocks, keys),
                scales.T,
                up,
                outw,
            )
        ),
    )
    return pl.pallas_call(
        finish,
        out_shape=(
            jax.ShapeDtypeStruct((own, head_count * vhead), jnp.bfloat16),
            jax.ShapeDtypeStruct((n // heads, columns), jnp.bfloat16),
        ),
        in_specs=[vmem] * 3,
        out_specs=(vmem, vmem),
        compiler_params=pltpu.CompilerParams(vmem_limit_bytes=1024 * 1024),
        name="finish",
    )(attention, summed, out_scales)


def solution(mesh):
    ctx, heads = mesh.shape["ctx"], mesh.shape["head"]
    return jax.shard_map(
        functools.partial(block, ctx, heads),
        mesh=mesh,
        in_specs=(
            P(("groups", "ctx"), "head", None),
            P(("groups", "ctx"), None),
            P(("groups", "ctx"), None),
            P(("groups", "ctx")),
            P("groups"),
            P("head", None, None),
            P("head", "ctx"),
            P("ctx"),
        ),
        out_specs=(P(("groups", "ctx"), "head"), P(("groups", "head"), "ctx")),
        check_vma=False,
    )
```
